8 devices in a mesh: dp: 1 (over z), tp: 2 (over y), sp: 4 (over x, core).
Axes of the slice: x: 2, y: 2, z: 1, core: 2. Of those that a mesh axis runs over, the one named last changes fastest.
Arguments:
- hidden: bfloat16 [128, 8192], P('dp')
- lengths: int32 [128], P('dp')
- k_cache: bfloat16 [128, 1024, 8, 128], P('dp', 'sp', 'tp')
- v_cache: bfloat16 [128, 1024, 8, 128], P('dp', 'sp', 'tp')
- norm_gain: bfloat16 [8192], replicated
- w_q: bfloat16 [8192, 8192], P(None, 'tp')
- w_k: bfloat16 [8192, 1024], P(None, 'tp')
- w_v: bfloat16 [8192, 1024], P(None, 'tp')
- w_o: bfloat16 [8192, 8192], P('tp')
- inv_freq: float32 [64], replicated
Outputs:
- output 1: bfloat16 [128, 8192], P('dp')
- output 2: bfloat16 [128, 1024, 8, 128], P('dp', 'sp', 'tp')
- output 3: bfloat16 [128, 1024, 8, 128], P('dp', 'sp', 'tp')
All inputs are finite; a program needn't handle non-finite values.
Results may differ from the reference program's by a relative error of at most 0.0085197.
Values sent between devices are 32-bit elements.
A program may use at most 1.25 GiB of HBM per device.

```python
import jax
import jax.numpy as jnp
from jax import lax

BATCH = 128
MODEL_DIM = 8192
NUM_HEADS = 64
KV_HEADS = 8
HEAD_DIM = 128
CACHE_LEN = 1024

NORM_EPS = 1e-5
ROPE_BASE = 500000.0


def setup_inputs(seed: int = 0, part: int = 0) -> dict:
    part_key = jax.random.fold_in(jax.random.key(seed), part)
    key_list = jax.random.split(part_key, 5)
    len_keys = jax.random.split(jax.random.fold_in(part_key, 3), 4)
    shared = jax.random.split(jax.random.key(seed + 1), 6)
    hidden = 0.5 * jax.random.normal(key_list[0], (BATCH, MODEL_DIM), jnp.float32)
    long_len = jax.random.randint(len_keys[0], (BATCH,), 0, CACHE_LEN)
    short_len = jax.random.randint(len_keys[1], (BATCH,), 0, 8)
    pick_short = jax.random.randint(len_keys[2], (BATCH,), 0, 4) == 0
    perm_ids = jax.random.permutation(len_keys[3], BATCH)
    lengths = jnp.where(pick_short, short_len, long_len)
    lengths = lengths.at[perm_ids[0]].set(CACHE_LEN - 1).at[perm_ids[1]].set(0).astype(jnp.int32)
    k_cache = jax.random.normal(key_list[1], (BATCH, CACHE_LEN, KV_HEADS, HEAD_DIM), jnp.float32)
    seg_count = 64
    seg_ids = jnp.arange(CACHE_LEN) * seg_count // CACHE_LEN
    seg_means = jax.random.normal(key_list[2], (BATCH, seg_count, KV_HEADS, HEAD_DIM), jnp.float32)
    v_noise = jax.random.normal(key_list[3], (BATCH, CACHE_LEN, KV_HEADS, HEAD_DIM), jnp.float32)
    v_cache = 3.0 * seg_means[:, seg_ids] + v_noise
    norm_gain = 1.0 + 0.3 * jax.random.normal(shared[0], (MODEL_DIM,), jnp.float32)
    w_q = jax.random.normal(shared[1], (MODEL_DIM, NUM_HEADS * HEAD_DIM), jnp.float32) * MODEL_DIM ** -0.5
    w_k = jax.random.normal(shared[2], (MODEL_DIM, KV_HEADS * HEAD_DIM), jnp.float32) * MODEL_DIM ** -0.5
    w_v = jax.random.normal(shared[3], (MODEL_DIM, KV_HEADS * HEAD_DIM), jnp.float32) * MODEL_DIM ** -0.5
    w_o = jax.random.normal(shared[4], (NUM_HEADS * HEAD_DIM, MODEL_DIM), jnp.float32) * (NUM_HEADS * HEAD_DIM) ** -0.5
    exponent = jnp.arange(0, HEAD_DIM, 2).astype(jnp.float32) / HEAD_DIM
    jitter = jnp.exp(0.2 * jax.random.uniform(shared[5], (HEAD_DIM // 2,), jnp.float32, minval=-1.0, maxval=1.0))
    inv_freq = jnp.power(ROPE_BASE, -exponent) * jitter
    return {
        'hidden': hidden.astype(jnp.bfloat16),
        'lengths': lengths,
        'k_cache': k_cache.astype(jnp.bfloat16),
        'v_cache': v_cache.astype(jnp.bfloat16),
        'norm_gain': norm_gain.astype(jnp.bfloat16),
        'w_q': w_q.astype(jnp.bfloat16),
        'w_k': w_k.astype(jnp.bfloat16),
        'w_v': w_v.astype(jnp.bfloat16),
        'w_o': w_o.astype(jnp.bfloat16),
        'inv_freq': inv_freq.astype(jnp.float32),
    }


def rms_norm(hidden, norm_gain):
    hidden_f32 = hidden.astype(jnp.float32)
    inv_rms = lax.rsqrt(jnp.mean(hidden_f32 * hidden_f32, axis=-1, keepdims=True) + NORM_EPS)
    return (hidden_f32 * inv_rms * norm_gain.astype(jnp.float32)).astype(jnp.bfloat16)


def apply_rope(head_vec, angles):
    half_dim = head_vec.shape[-1] // 2
    vec_f32 = head_vec.astype(jnp.float32)
    cos_ang = jnp.cos(angles)[:, None, :]
    sin_ang = jnp.sin(angles)[:, None, :]
    lo_half = vec_f32[..., :half_dim]
    hi_half = vec_f32[..., half_dim:]
    rotated = jnp.concatenate([lo_half * cos_ang - hi_half * sin_ang, hi_half * cos_ang + lo_half * sin_ang], axis=-1)
    return rotated.astype(jnp.bfloat16)


def reference(hidden, lengths, k_cache, v_cache, norm_gain, w_q, w_k, w_v, w_o, inv_freq):
    normed = rms_norm(hidden, norm_gain)
    q_heads = jnp.dot(normed, w_q, preferred_element_type=jnp.float32).astype(jnp.bfloat16).reshape(BATCH, NUM_HEADS, HEAD_DIM)
    k_new = jnp.dot(normed, w_k, preferred_element_type=jnp.float32).astype(jnp.bfloat16).reshape(BATCH, KV_HEADS, HEAD_DIM)
    v_new = jnp.dot(normed, w_v, preferred_element_type=jnp.float32).astype(jnp.bfloat16).reshape(BATCH, KV_HEADS, HEAD_DIM)
    angles = lengths.astype(jnp.float32)[:, None] * inv_freq[None, :]
    q_rot = apply_rope(q_heads, angles)
    k_rot = apply_rope(k_new, angles)
    row_ids = jnp.arange(BATCH)
    k_out = k_cache.at[row_ids, lengths].set(k_rot)
    v_out = v_cache.at[row_ids, lengths].set(v_new)
    group_size = NUM_HEADS // KV_HEADS
    q_grp = q_rot.reshape(BATCH, KV_HEADS, group_size, HEAD_DIM)
    score_scale = HEAD_DIM ** -0.5

    def one_seq(seq_args):
        q_one, k_one, v_one, len_one = seq_args
        scores = jnp.einsum('kgd,skd->kgs', q_one.astype(jnp.float32), k_one.astype(jnp.float32)) * score_scale
        valid_mask = jnp.arange(CACHE_LEN) <= len_one
        scores = jnp.where(valid_mask, scores, -jnp.inf)
        top_score = jnp.max(scores, axis=-1, keepdims=True)
        weights = jnp.where(valid_mask, jnp.exp(scores - top_score), 0.0)
        weight_sum = jnp.sum(weights, axis=-1)
        weighted = jnp.einsum('kgs,skd->kgd', weights.astype(jnp.bfloat16).astype(jnp.float32), v_one.astype(jnp.float32))
        return (weighted / weight_sum[..., None]).astype(jnp.bfloat16)

    attn_out = lax.map(one_seq, (q_grp, k_out, v_out, lengths))
    attn_flat = attn_out.reshape(BATCH, NUM_HEADS * HEAD_DIM)
    proj_out = jnp.dot(attn_flat, w_o, preferred_element_type=jnp.float32)
    y_out = (hidden.astype(jnp.float32) + proj_out).astype(jnp.bfloat16)
    return (y_out, k_out, v_out)
```

```python
import functools

import jax
import jax.numpy as jnp
from jax import lax
from jax.experimental import pallas as pl
from jax.experimental.pallas import tpu as pltpu
from jax.sharding import PartitionSpec as P

NORM_EPS = 1e-5
NEG_BIG = -3.0e38
LOG2E = 1.4426950408889634
ANY = pl.BlockSpec(memory_space=pl.ANY)
VMEM = pl.BlockSpec(memory_space=pltpu.VMEM)
SMEM = pl.BlockSpec(memory_space=pltpu.SMEM)


def rms_norm(hidden, norm_gain):
    hidden_f32 = hidden.astype(jnp.float32)
    inv_rms = lax.rsqrt(jnp.mean(hidden_f32 * hidden_f32, axis=-1, keepdims=True) + NORM_EPS)
    return (hidden_f32 * inv_rms * norm_gain.astype(jnp.float32)).astype(jnp.bfloat16)


def apply_rope(head_vec, angles):
    half_dim = head_vec.shape[-1] // 2
    vec_f32 = head_vec.astype(jnp.float32)
    cos_ang = jnp.cos(angles)[:, None, :]
    sin_ang = jnp.sin(angles)[:, None, :]
    lo_half = vec_f32[..., :half_dim]
    hi_half = vec_f32[..., half_dim:]
    rotated = jnp.concatenate([lo_half * cos_ang - hi_half * sin_ang, hi_half * cos_ang + lo_half * sin_ang], axis=-1)
    return rotated.astype(jnp.bfloat16)


CHUNK = 8
NBUF = 6
LAG = 3


def attend_kernel(len_ref, q_ref, kv_ref, k_hbm, v_hbm, ko_hbm, vo_hbm, o_ref, st_ref,
                  kbuf, vbuf, obuf, mbuf, lbuf, in_sem, out_sem):
    batch, rows, head_dim = k_hbm.shape
    kv_local = kv_ref.shape[0] * kv_ref.shape[2] // 2
    heads = q_ref.shape[0] * q_ref.shape[2]
    slots = rows // kv_local
    steps = batch // CHUNK
    slot_start = lax.axis_index('sp') * slots

    def copies_in(i):
        b = lax.rem(i, NBUF)
        src = pl.ds(i * CHUNK, CHUNK)
        return (pltpu.make_async_copy(k_hbm.at[src], kbuf.at[b], in_sem.at[0, b]),
                pltpu.make_async_copy(v_hbm.at[src], vbuf.at[b], in_sem.at[1, b]))

    def copies_out(i):
        b = lax.rem(i, NBUF)
        dst = pl.ds(i * CHUNK, CHUNK)
        return (pltpu.make_async_copy(kbuf.at[b], ko_hbm.at[dst], out_sem.at[0, b]),
                pltpu.make_async_copy(vbuf.at[b], vo_hbm.at[dst], out_sem.at[1, b]))

    for i in range(NBUF - LAG):
        for c in copies_in(i):
            c.start()

    col = lax.broadcasted_iota(jnp.int32, (heads, rows), 1)
    row = lax.broadcasted_iota(jnp.int32, (heads, rows), 0)
    head_ok = lax.rem(col, kv_local) == row // (heads // kv_local)
    tile_slot = lax.broadcasted_iota(jnp.int32, (16, head_dim), 0) // kv_local
    lane = lax.broadcasted_iota(jnp.int32, (heads, batch), 1)
    score_scale = head_dim ** -0.5 * LOG2E

    def step(i, carry):
        buf = lax.rem(i, NBUF)

        @pl.when((i >= LAG) & (i + NBUF - LAG < steps))
        def _():
            for c in copies_out(i - LAG):
                c.wait()

        @pl.when(i + NBUF - LAG < steps)
        def _():
            for c in copies_in(i + NBUF - LAG):
                c.start()

        for c in copies_in(i):
            c.wait()
        for s in range(CHUNK):
            b = i * CHUNK + s
            pos = len_ref[b] - slot_start
            own = (pos >= 0) & (pos < slots)
            safe = jnp.where(own, pos, 0)
            per_tile = 16 // kv_local
            base = pl.multiple_of(safe // per_tile * 16, 16)
            pick = (tile_slot == lax.rem(safe, per_tile)) & own
            new0 = kv_ref[0, b]
            new1 = kv_ref[1, b]
            for dst, lo in ((kbuf, 0), (vbuf, kv_local // 2)):
                new = jnp.concatenate([new0[lo:lo + kv_local // 2], new1[lo:lo + kv_local // 2]] * per_tile, axis=0)
                old = dst[buf, s, pl.ds(base, 16), :].astype(jnp.float32)
                dst[buf, s, pl.ds(base, 16), :] = jnp.where(pick, new, old).astype(jnp.bfloat16)
        m_all, l_all = mbuf[...], lbuf[...]
        for s in range(0, CHUNK, 2):
            b0 = i * CHUNK + s
            b1 = b0 + 1
            limit0 = (len_ref[b0] - slot_start + 1) * kv_local
            limit1 = (len_ref[b1] - slot_start + 1) * kv_local
            q0 = jnp.concatenate([q_ref[0, b0], q_ref[1, b0]], axis=0).astype(jnp.bfloat16)
            q1 = jnp.concatenate([q_ref[0, b1], q_ref[1, b1]], axis=0).astype(jnp.bfloat16)
            zero = jnp.zeros_like(q0)
            q = jnp.concatenate([jnp.concatenate([q0, zero], axis=1), jnp.concatenate([zero, q1], axis=1)], axis=0)
            k = jnp.concatenate([kbuf[buf, s], kbuf[buf, s + 1]], axis=1)
            v = jnp.concatenate([vbuf[buf, s], vbuf[buf, s + 1]], axis=1)
            scores = lax.dot_general(q, k, (((1,), (1,)), ((), ())), preferred_element_type=jnp.float32)
            valid = jnp.concatenate([head_ok & (col < limit0), head_ok & (col < limit1)], axis=0)
            scores = jnp.where(valid, scores * score_scale, NEG_BIG)
            top = jnp.max(scores, axis=-1, keepdims=True)
            weights = jnp.where(valid, jnp.exp2(scores - top), 0.0)
            total = jnp.sum(weights, axis=-1, keepdims=True)
            out = jnp.dot(weights.astype(jnp.bfloat16), v, preferred_element_type=jnp.float32)
            obuf[s] = out[:heads, :head_dim]
            obuf[s + 1] = out[heads:, head_dim:]
            m_all = jnp.where(lane == b0, top[:heads], jnp.where(lane == b1, top[heads:], m_all))
            l_all = jnp.where(lane == b0, total[:heads], jnp.where(lane == b1, total[heads:], l_all))
        mbuf[...] = m_all
        lbuf[...] = l_all
        o_ref[:, pl.ds(pl.multiple_of(i * CHUNK, CHUNK), CHUNK), :] = jnp.swapaxes(obuf[...], 0, 1)
        for c in copies_out(i):
            c.start()

        return carry

    mbuf[...] = jnp.zeros_like(mbuf)
    lbuf[...] = jnp.zeros_like(lbuf)
    lax.fori_loop(0, steps, step, 0)
    for i in range(steps - NBUF, steps):
        for c in copies_out(i):
            c.wait()
    st_ref[0] = mbuf[...].T
    st_ref[1] = lbuf[...].T


def write_and_attend(lengths, q_all, kv_all, k_cache, v_cache):
    batch, slots, kv_local, head_dim = k_cache.shape
    heads = q_all.shape[0] * q_all.shape[2]
    rows = slots * kv_local
    flat = (batch, rows, head_dim)
    out_shape = (jax.ShapeDtypeStruct(flat, k_cache.dtype), jax.ShapeDtypeStruct(flat, v_cache.dtype),
                 jax.ShapeDtypeStruct((heads, batch, head_dim), jnp.float32),
                 jax.ShapeDtypeStruct((2, batch, heads), jnp.float32))
    k_new, v_new, o, stats = pl.pallas_call(
        attend_kernel,
        out_shape=out_shape,
        in_specs=[SMEM, VMEM, VMEM, ANY, ANY],
        out_specs=(ANY, ANY, VMEM, VMEM),
        scratch_shapes=[
            pltpu.VMEM((NBUF, CHUNK, rows, head_dim), jnp.bfloat16),
            pltpu.VMEM((NBUF, CHUNK, rows, head_dim), jnp.bfloat16),
            pltpu.VMEM((CHUNK, heads, head_dim), jnp.float32),
            pltpu.VMEM((heads, batch), jnp.float32),
            pltpu.VMEM((heads, batch), jnp.float32),
            pltpu.SemaphoreType.DMA((2, NBUF)),
            pltpu.SemaphoreType.DMA((2, NBUF)),
        ],
        compiler_params=pltpu.CompilerParams(vmem_limit_bytes=56 * 1024 * 1024),
        cost_estimate=pl.CostEstimate(flops=4 * batch * heads * rows * head_dim, bytes_accessed=8 * batch * rows * head_dim, transcendentals=0),
        name='attend',
    )(lengths, q_all, kv_all, k_cache.reshape(flat), v_cache.reshape(flat))
    return k_new.reshape(k_cache.shape), v_new.reshape(v_cache.shape), o, stats


PIECES = 4
MESH = pl.DeviceIdType.MESH


def combine_kernel(o_ref, st_ref, w_hbm, hid_hbm, y_ref, w, hid, r1, st1, c1, stc, r2, st2, att, lhs, part, r3, yall,
                   w_sem, send, recv):
    heads, batch, head_dim = o_ref.shape
    half = heads // 2
    cols = part.shape[2]
    rows = batch // PIECES
    sp, y = lax.axis_index('sp'), lax.axis_index('tp')
    c, x = lax.rem(sp, 2), sp // 2
    to_c, to_x, to_y = {'sp': sp + 1 - 2 * c}, {'sp': sp + 2 - 4 * x}, {'tp': 1 - y}
    block = lambda xx, cc, yy: 4 * xx + 2 * cc + yy
    mine = block(x, c, y)

    barrier = pltpu.get_barrier_semaphore()
    for dev in (to_c, to_x, to_y):
        pl.semaphore_signal(barrier, inc=1, device_id=dev, device_id_type=MESH)

    w_copies = [pltpu.make_async_copy(w_hbm.at[:, pl.ds(pl.multiple_of((2 * sp + h) * cols, cols), cols)], w.at[h], w_sem.at[h]) for h in range(2)]
    hid_copy = pltpu.make_async_copy(hid_hbm.at[:, pl.ds(pl.multiple_of(mine * cols, cols), cols)], hid, w_sem.at[2])
    hid_copy.start()
    for cp in w_copies:
        cp.start()
    pl.semaphore_wait(barrier, 3)

    def copy(kind, j, src, dst, dev):
        return pltpu.make_async_remote_copy(src_ref=src, dst_ref=dst, send_sem=send.at[kind, j], recv_sem=recv.at[kind, j], device_id=dev, device_id_type=MESH)

    def at(j):
        return pl.ds(j * rows, rows)

    pending = []

    def push(cp):
        cp.start()
        pending.append(cp)

    stat_c = copy(0, 0, st_ref, st1, to_c)
    push(stat_c)
    o_copies = [copy(1, j, o_ref.at[pl.ds((1 - c) * half, half), at(j)], r1.at[:, at(j)], to_c) for j in range(PIECES)]
    for cp in o_copies:
        push(cp)

    def pick_half(a):
        return jnp.where(c == 0, a[:, :half], a[:, half:])

    stat_c.wait_recv()
    m_a, l_a, m_b, l_b = (pick_half(v) for v in (st_ref[0], st_ref[1], st1[0], st1[1]))
    top = jnp.maximum(m_a, m_b)
    f_a, f_b = jnp.exp2(m_a - top), jnp.exp2(m_b - top)
    stc[0] = top
    stc[1] = l_a * f_a + l_b * f_b
    stat_x = copy(2, 0, stc, st2, to_x)
    push(stat_x)
    x_copies = [copy(3, j, c1.at[:, at(j)], r2.at[:, at(j)], to_x) for j in range(PIECES)]
    for j in range(PIECES):
        o_copies[j].wait_recv()
        lo = j * rows
        for h in range(half):
            c1[h, at(j)] = o_ref[c * half + h, at(j)] * f_a[lo:lo + rows, h:h + 1] + r1[h, at(j)] * f_b[lo:lo + rows, h:h + 1]
        push(x_copies[j])

    stat_x.wait_recv()
    m_a, l_a, m_b, l_b = stc[0], stc[1], st2[0], st2[1]
    top = jnp.maximum(m_a, m_b)
    g_a, g_b = jnp.exp2(m_a - top), jnp.exp2(m_b - top)
    inv = 1.0 / (l_a * g_a + l_b * g_b)
    g_a, g_b = g_a * inv, g_b * inv

    own_att = att.at[pl.ds(c * half, half)]
    att_copies = [copy(4, j, own_att.at[:, at(j)], own_att.at[:, at(j)], to_c) for j in range(PIECES)]
    part_copies = [copy(5, j, part.at[1 - y, at(j)], r3.at[at(j)], to_y) for j in range(PIECES)]

    def spread(kind, j, blk, dev):
        return copy(kind, j, yall.at[blk, at(j)], yall.at[blk, at(j)], dev)

    b_x, b_y, b_xy = block(1 - x, c, y), block(x, c, 1 - y), block(1 - x, c, 1 - y)

    def finish_heads(j):
        x_copies[j].wait_recv()
        lo = j * rows
        for h in range(half):
            att[c * half + h, at(j)] = c1[h, at(j)] * g_a[lo:lo + rows, h:h + 1] + r2[h, at(j)] * g_b[lo:lo + rows, h:h + 1]
        push(att_copies[j])

    def multiply(j):
        if j == 0:
            for cp in w_copies:
                cp.wait()
        att_copies[j].wait_recv()
        for h in range(heads):
            lhs[:, h * head_dim:(h + 1) * head_dim] = att[h, at(j)].astype(jnp.bfloat16)

        def tiles(side):
            def tile(n, carry):
                sl = pl.ds(pl.multiple_of(n * 256, 256), 256)
                part[side, at(j), sl] = jnp.dot(lhs[...], w[side, :, sl], preferred_element_type=jnp.float32)
                return carry
            lax.fori_loop(0, cols // 256, tile, 0)

        tiles(1 - y)
        push(part_copies[j])
        tiles(y)

    def finish_sum(j):
        if j == 0:
            hid_copy.wait()
        part_copies[j].wait_recv()
        yall[mine, at(j)] = hid[at(j)].astype(jnp.float32) + (part[y, at(j)] + r3[at(j)])
        push(spread(7, j, mine, to_x))
        push(spread(8, j, mine, to_y))
        push(spread(6, j, mine, to_c))

    def forward(j):
        spread(7, j, b_x, to_x).wait_recv()
        push(spread(10, j, b_x, to_y))
        push(spread(9, j, b_x, to_c))
        spread(8, j, b_y, to_y).wait_recv()
        push(spread(11, j, b_y, to_c))

    def forward_last(j):
        spread(10, j, b_xy, to_y).wait_recv()
        push(spread(12, j, b_xy, to_c))

    def emit(j):
        spread(6, j, block(x, 1 - c, y), to_c).wait_recv()
        spread(9, j, block(1 - x, 1 - c, y), to_c).wait_recv()
        spread(11, j, block(x, 1 - c, 1 - y), to_c).wait_recv()
        spread(12, j, block(1 - x, 1 - c, 1 - y), to_c).wait_recv()
        for g in range(8):
            y_ref[at(j), g * cols:(g + 1) * cols] = yall[g, at(j)].astype(y_ref.dtype)

    stages = ((finish_heads, 0), (finish_sum, 1), (multiply, 0), (forward, 2), (forward_last, 3), (emit, 4))
    for t in range(PIECES + 4):
        for stage, lag in stages:
            if 0 <= t - lag < PIECES:
                stage(t - lag)
    for cp in pending:
        cp.wait_send()


def combine_and_project(o, stats, w_o, hidden):
    heads, batch, head_dim = o.shape
    cols = w_o.shape[1] // 8
    half = heads // 2
    f32 = jnp.float32
    return pl.pallas_call(
        combine_kernel,
        out_shape=jax.ShapeDtypeStruct(hidden.shape, hidden.dtype),
        in_specs=[VMEM, VMEM, ANY, ANY],
        out_specs=VMEM,
        scratch_shapes=[
            pltpu.VMEM((2, w_o.shape[0], cols), w_o.dtype),
            pltpu.VMEM((batch, cols), hidden.dtype),
            pltpu.VMEM((half, batch, head_dim), f32),
            pltpu.VMEM(stats.shape, f32),
            pltpu.VMEM((half, batch, head_dim), f32),
            pltpu.VMEM((2, batch, half), f32),
            pltpu.VMEM((half, batch, head_dim), f32),
            pltpu.VMEM((2, batch, half), f32),
            pltpu.VMEM((heads, batch, head_dim), f32),
            pltpu.VMEM((batch // PIECES, heads * head_dim), jnp.bfloat16),
            pltpu.VMEM((2, batch, cols), f32),
            pltpu.VMEM((batch, cols), f32),
            pltpu.VMEM((8, batch, cols), f32),
            pltpu.SemaphoreType.DMA((3,)),
            pltpu.SemaphoreType.DMA((13, PIECES)),
            pltpu.SemaphoreType.DMA((13, PIECES)),
        ],
        compiler_params=pltpu.CompilerParams(collective_id=1, has_side_effects=True, vmem_limit_bytes=56 * 1024 * 1024),
        name='combine',
    )(o, stats, w_o, hidden)


def project(hidden, lengths, norm_gain, w_q, w_k, w_v, inv_freq):
    batch_size = hidden.shape[0]
    head_dim = 2 * inv_freq.shape[0]
    normed = rms_norm(hidden, norm_gain)
    q_heads = jnp.dot(normed, w_q, preferred_element_type=jnp.float32).astype(jnp.bfloat16).reshape(batch_size, -1, head_dim)
    k_new = jnp.dot(normed, w_k, preferred_element_type=jnp.float32).astype(jnp.bfloat16).reshape(batch_size, -1, head_dim)
    v_new = jnp.dot(normed, w_v, preferred_element_type=jnp.float32).astype(jnp.bfloat16).reshape(batch_size, -1, head_dim)
    angles = lengths.astype(jnp.float32)[:, None] * inv_freq[None, :]
    q = apply_rope(q_heads, angles).astype(jnp.float32)
    k = apply_rope(k_new, angles).astype(jnp.float32)
    v = v_new.astype(jnp.float32)
    h = q.shape[1] // 2
    g = k.shape[1] // 2
    q_all = jnp.stack([q[:, :h], q[:, h:]])
    kv_all = jnp.stack([jnp.concatenate([k[:, :g], v[:, :g]], 1), jnp.concatenate([k[:, g:], v[:, g:]], 1)])
    return q_all, kv_all


def device_step(hidden, lengths, k_cache, v_cache, norm_gain, w_q, w_k, w_v, w_o, inv_freq):
    q_all, kv_all = project(hidden, lengths, norm_gain, w_q, w_k, w_v, inv_freq)
    k_upd, v_upd, o, stats = write_and_attend(lengths, q_all, kv_all, k_cache, v_cache)
    y_out = combine_and_project(o, stats, w_o, hidden)
    return y_out, k_upd, v_upd


def solution(mesh):
    cache_spec = P('dp', 'sp', 'tp', None)
    in_specs = (P('dp', None), P('dp'), cache_spec, cache_spec, P(None), P(None, 'tp'), P(None, 'tp'), P(None, 'tp'), P('tp', None), P(None))
    out_specs = (P('dp', None), cache_spec, cache_spec)
    return jax.shard_map(device_step, mesh=mesh, in_specs=in_specs, out_specs=out_specs, check_vma=False)
```

```python
import functools

import jax
import jax.numpy as jnp
from jax import lax
from jax.experimental import pallas as pl
from jax.experimental.pallas import tpu as pltpu
from jax.sharding import PartitionSpec as P

NORM_EPS = 1e-5
NEG_BIG = -3.0e38
LOG2E = 1.4426950408889634
ANY = pl.BlockSpec(memory_space=pl.ANY)
VMEM = pl.BlockSpec(memory_space=pltpu.VMEM)
SMEM = pl.BlockSpec(memory_space=pltpu.SMEM)


CHUNK = 8
NBUF = 6
LAG = 3


def attend_kernel(first, count, len_ref, q_ref, kv_ref, k_hbm, v_hbm, *refs):
    ko_hbm, vo_hbm, own_ref, oth_ref, kbuf, vbuf, obuf, mbuf, lbuf, in_sem, out_sem = refs[-11:]
    batch, rows, head_dim = k_hbm.shape
    kv_local = kv_ref.shape[2]
    heads = q_ref.shape[0] * q_ref.shape[2]
    slots = rows // kv_local
    steps = count // CHUNK
    slot_start = lax.axis_index('sp') * slots

    def copies_in(i):
        b = lax.rem(i, NBUF)
        src = pl.ds(first + i * CHUNK, CHUNK)
        return (pltpu.make_async_copy(k_hbm.at[src], kbuf.at[b], in_sem.at[0, b]),
                pltpu.make_async_copy(v_hbm.at[src], vbuf.at[b], in_sem.at[1, b]))

    def copies_out(i):
        b = lax.rem(i, NBUF)
        dst = pl.ds(first + i * CHUNK, CHUNK)
        return (pltpu.make_async_copy(kbuf.at[b], ko_hbm.at[dst], out_sem.at[0, b]),
                pltpu.make_async_copy(vbuf.at[b], vo_hbm.at[dst], out_sem.at[1, b]))

    for i in range(NBUF - LAG):
        for c in copies_in(i):
            c.start()

    col = lax.broadcasted_iota(jnp.int32, (heads, rows), 1)
    row = lax.broadcasted_iota(jnp.int32, (heads, rows), 0)
    head_ok = lax.rem(col, kv_local) == row // (heads // kv_local)
    tile_slot = lax.broadcasted_iota(jnp.int32, (16, head_dim), 0) // kv_local
    lane = lax.broadcasted_iota(jnp.int32, (heads, batch), 1)
    score_scale = head_dim ** -0.5 * LOG2E
    half = heads // 2
    core = lax.rem(lax.axis_index('sp'), 2)

    def step(i, carry):
        buf = lax.rem(i, NBUF)

        @pl.when((i >= LAG) & (i + NBUF - LAG < steps))
        def _():
            for c in copies_out(i - LAG):
                c.wait()

        @pl.when(i + NBUF - LAG < steps)
        def _():
            for c in copies_in(i + NBUF - LAG):
                c.start()

        for c in copies_in(i):
            c.wait()
        for s in range(CHUNK):
            b = first + i * CHUNK + s
            pos = len_ref[b] - slot_start
            own = (pos >= 0) & (pos < slots)
            safe = jnp.where(own, pos, 0)
            per_tile = 16 // kv_local
            base = pl.multiple_of(safe // per_tile * 16, 16)
            pick = (tile_slot == lax.rem(safe, per_tile)) & own
            for dst, which in ((kbuf, 0), (vbuf, 1)):
                new = jnp.concatenate([kv_ref[which, b]] * per_tile, axis=0)
                old = dst[buf, s, pl.ds(base, 16), :].astype(jnp.float32)
                dst[buf, s, pl.ds(base, 16), :] = jnp.where(pick, new, old).astype(jnp.bfloat16)
        m_all, l_all = mbuf[...], lbuf[...]
        for s in range(0, CHUNK, 2):
            b0 = first + i * CHUNK + s
            b1 = b0 + 1
            limit0 = (len_ref[b0] - slot_start + 1) * kv_local
            limit1 = (len_ref[b1] - slot_start + 1) * kv_local
            q0 = jnp.concatenate([q_ref[0, b0], q_ref[1, b0]], axis=0).astype(jnp.bfloat16)
            q1 = jnp.concatenate([q_ref[0, b1], q_ref[1, b1]], axis=0).astype(jnp.bfloat16)
            zero = jnp.zeros_like(q0)
            q = jnp.concatenate([jnp.concatenate([q0, zero], axis=1), jnp.concatenate([zero, q1], axis=1)], axis=0)
            k = jnp.concatenate([kbuf[buf, s], kbuf[buf, s + 1]], axis=1)
            v = jnp.concatenate([vbuf[buf, s], vbuf[buf, s + 1]], axis=1)
            scores = lax.dot_general(q, k, (((1,), (1,)), ((), ())), preferred_element_type=jnp.float32)
            valid = jnp.concatenate([head_ok & (col < limit0), head_ok & (col < limit1)], axis=0)
            scores = jnp.where(valid, scores * score_scale, NEG_BIG)
            top = jnp.max(scores, axis=-1, keepdims=True)
            weights = jnp.where(valid, jnp.exp2(scores - top), 0.0)
            total = jnp.sum(weights, axis=-1, keepdims=True)
            out = jnp.dot(weights.astype(jnp.bfloat16), v, preferred_element_type=jnp.float32)
            obuf[s] = out[:heads, :head_dim]
            obuf[s + 1] = out[heads:, head_dim:]
            m_all = jnp.where(lane == b0, top[:heads], jnp.where(lane == b1, top[heads:], m_all))
            l_all = jnp.where(lane == b0, total[:heads], jnp.where(lane == b1, total[heads:], l_all))
        mbuf[...] = m_all
        lbuf[...] = l_all
        out_rows = pl.ds(pl.multiple_of(i * CHUNK, CHUNK), CHUNK)
        by_head = jnp.swapaxes(obuf[...], 0, 1)
        own_ref[:half, out_rows] = jnp.where(core == 0, by_head[:half], by_head[half:])
        oth_ref[:half, out_rows] = jnp.where(core == 0, by_head[half:], by_head[:half])
        for c in copies_out(i):
            c.start()

        return carry

    mbuf[...] = jnp.zeros_like(mbuf)
    lbuf[...] = jnp.zeros_like(lbuf)
    lax.fori_loop(0, steps, step, 0)
    for i in range(steps - NBUF, steps):
        for c in copies_out(i):
            c.wait()
    stats = []
    for lo in (0, half):
        rows_ml = [mbuf[lo:lo + half], lbuf[lo:lo + half], jnp.zeros((batch - 2 * half, batch), jnp.float32)]
        stats.append(jnp.concatenate(rows_ml, axis=0).T[first:first + count])
    own_ref[half] = jnp.where(core == 0, stats[0], stats[1])
    oth_ref[half] = jnp.where(core == 0, stats[1], stats[0])


def write_and_attend(first, count, lengths, q_all, kv_all, k_cache, v_cache, written=()):
    batch, rows, head_dim = k_cache.shape
    heads = q_all.shape[0] * q_all.shape[2]
    part = jax.ShapeDtypeStruct((heads // 2 + 1, count, head_dim), jnp.float32)
    cache = jax.ShapeDtypeStruct(k_cache.shape, k_cache.dtype)
    return pl.pallas_call(
        functools.partial(attend_kernel, first, count),
        out_shape=(cache, cache, part, part),
        in_specs=[SMEM, VMEM, VMEM, ANY, ANY] + [ANY] * len(written),
        out_specs=(ANY, ANY, VMEM, VMEM),
        input_output_aliases={5: 0, 6: 1} if written else {},
        scratch_shapes=[
            pltpu.VMEM((NBUF, CHUNK, rows, head_dim), jnp.bfloat16),
            pltpu.VMEM((NBUF, CHUNK, rows, head_dim), jnp.bfloat16),
            pltpu.VMEM((CHUNK, heads, head_dim), jnp.float32),
            pltpu.VMEM((heads, batch), jnp.float32),
            pltpu.VMEM((heads, batch), jnp.float32),
            pltpu.SemaphoreType.DMA((2, NBUF)),
            pltpu.SemaphoreType.DMA((2, NBUF)),
        ],
        compiler_params=pltpu.CompilerParams(vmem_limit_bytes=34 * 1024 * 1024),
        cost_estimate=pl.CostEstimate(flops=100 * count * heads * rows * head_dim, bytes_accessed=8 * count * rows * head_dim, transcendentals=0),
        name='attend',
    )(lengths, q_all, kv_all, k_cache, v_cache, *written)


FIRST = 64
B_PIECES = 2
MESH = pl.DeviceIdType.MESH


def weigh(tiles):
    half = 16
    tops = [t[:, :half] for t in tiles]
    top = functools.reduce(jnp.maximum, tops)
    scales = [jnp.exp2(m - top) for m in tops]
    total = sum(t[:, half:2 * half] * s for t, s in zip(tiles, scales))
    return top, total, scales


def combine_kernel(own_a, core_a, x_a, diag_a, own_b, oth_b, w_hbm, hid_hbm, y_ref, w, hid, r1, c1, r2, att, lhs, part, r3, yall,
                   w_sem, send, recv):
    heads, batch, head_dim = att.shape
    half = heads // 2
    cols = part.shape[2]
    first = own_a.shape[1]
    piece_rows = own_b.shape[1] // B_PIECES
    pieces = [(0, first)] + [(first + j * piece_rows, piece_rows) for j in range(B_PIECES)]
    sp, y = lax.axis_index('sp'), lax.axis_index('tp')
    c, x = lax.rem(sp, 2), sp // 2
    to_c, to_x, to_y = {'sp': sp + 1 - 2 * c}, {'sp': sp + 2 - 4 * x}, {'tp': 1 - y}
    block = lambda xx, cc, yy: 4 * xx + 2 * cc + yy
    mine = block(x, c, y)

    barrier = pltpu.get_barrier_semaphore()
    for dev in (to_c, to_x, to_y):
        pl.semaphore_signal(barrier, inc=1, device_id=dev, device_id_type=MESH)

    w_copies = [pltpu.make_async_copy(w_hbm.at[:, pl.ds(pl.multiple_of((2 * sp + h) * cols, cols), cols)], w.at[h], w_sem.at[h]) for h in range(2)]
    hid_copy = pltpu.make_async_copy(hid_hbm.at[:, pl.ds(pl.multiple_of(mine * cols, cols), cols)], hid, w_sem.at[2])
    hid_copy.start()
    for cp in w_copies:
        cp.start()
    pl.semaphore_wait(barrier, 3)

    def copy(kind, j, src, dst, dev):
        return pltpu.make_async_remote_copy(src_ref=src, dst_ref=dst, send_sem=send.at[kind, j], recv_sem=recv.at[kind, j], device_id=dev, device_id_type=MESH)

    def at(j):
        return pl.ds(*pieces[j])

    def local(j):
        return pl.ds(pieces[j][0] - first, pieces[j][1])

    pending = []

    def push(cp):
        cp.start()
        pending.append(cp)

    b_range = range(1, B_PIECES + 1)
    stat_c = copy(0, 0, oth_b.at[half], r1.at[half], to_c)
    push(stat_c)
    o_copies = {j: copy(1, j, oth_b.at[pl.ds(0, half), local(j)], r1.at[pl.ds(0, half), local(j)], to_c) for j in b_range}
    for j in b_range:
        push(o_copies[j])

    own_att = att.at[pl.ds(c * half, half)]
    att_copies = [copy(4, j, own_att.at[:, at(j)], own_att.at[:, at(j)], to_c) for j in range(B_PIECES + 1)]
    part_copies = [copy(5, j, part.at[1 - y, at(j)], r3.at[at(j)], to_y) for j in range(B_PIECES + 1)]

    parts_a = (own_a, core_a, x_a, diag_a)
    _, total, scales = weigh([p[half] for p in parts_a])
    scales = [s / total for s in scales]
    for h in range(half):
        att[c * half + h, at(0)] = sum(p[h] * s[:, h:h + 1] for p, s in zip(parts_a, scales))
    push(att_copies[0])

    stat_c.wait_recv()
    top, total, scales = weigh([own_b[half], r1[half]])
    c1[half] = jnp.concatenate([top, total, jnp.zeros((own_b.shape[1], head_dim - 2 * half), jnp.float32)], axis=1)
    stat_x = copy(2, 0, c1.at[half], r2.at[half], to_x)
    push(stat_x)
    x_copies = {j: copy(3, j, c1.at[pl.ds(0, half), local(j)], r2.at[pl.ds(0, half), local(j)], to_x) for j in b_range}
    for j in b_range:
        o_copies[j].wait_recv()
        lo, n = pieces[j][0] - first, pieces[j][1]
        for h in range(half):
            c1[h, local(j)] = own_b[h, local(j)] * scales[0][lo:lo + n, h:h + 1] + r1[h, local(j)] * scales[1][lo:lo + n, h:h + 1]
        push(x_copies[j])

    def spread(kind, j, blk, dev):
        return copy(kind, j, yall.at[blk, at(j)], yall.at[blk, at(j)], dev)

    b_x, b_y, b_xy = block(1 - x, c, y), block(x, c, 1 - y), block(1 - x, c, 1 - y)
    final = {}

    def finish_heads(j):
        if j == 0:
            return
        if j == 1:
            stat_x.wait_recv()
            _, tot, sc = weigh([c1[half], r2[half]])
            final['scales'] = [s / tot for s in sc]
        x_copies[j].wait_recv()
        lo, n = pieces[j][0] - first, pieces[j][1]
        for h in range(half):
            att[c * half + h, at(j)] = sum(p[h, local(j)] * s[lo:lo + n, h:h + 1] for p, s in zip((c1, r2), final['scales']))
        push(att_copies[j])

    def multiply(j):
        if j == 0:
            for cp in w_copies:
                cp.wait()
        att_copies[j].wait_recv()
        n = pieces[j][1]
        for h in range(heads):
            lhs[:n, h * head_dim:(h + 1) * head_dim] = att[h, at(j)].astype(jnp.bfloat16)

        def tiles(side):
            def tile(i, carry):
                sl = pl.ds(pl.multiple_of(i * 256, 256), 256)
                part[side, at(j), sl] = jnp.dot(lhs[:n], w[side, :, sl], preferred_element_type=jnp.float32)
                return carry
            lax.fori_loop(0, cols // 256, tile, 0)

        tiles(1 - y)
        push(part_copies[j])
        tiles(y)

    def finish_sum(j):
        if j == 0:
            hid_copy.wait()
        part_copies[j].wait_recv()
        yall[mine, at(j)] = hid[at(j)].astype(jnp.float32) + (part[y, at(j)] + r3[at(j)])
        push(spread(8, j, mine, to_y))
        push(spread(7, j, mine, to_x))
        push(spread(6, j, mine, to_c))

    def forward(j):
        def from_x():
            spread(7, j, b_x, to_x).wait_recv()
            if j:
                push(spread(10, j, b_x, to_y))
            push(spread(9, j, b_x, to_c))

        def from_y():
            spread(8, j, b_y, to_y).wait_recv()
            if not j:
                push(spread(10, j, b_y, to_x))
            push(spread(11, j, b_y, to_c))

        for take in (from_x, from_y) if j else (from_y, from_x):
            take()

    def forward_last(j):
        spread(10, j, b_xy, to_y).wait_recv()
        push(spread(12, j, b_xy, to_c))

    def emit(j):
        spread(6, j, block(x, 1 - c, y), to_c).wait_recv()
        spread(9, j, block(1 - x, 1 - c, y), to_c).wait_recv()
        spread(11, j, block(x, 1 - c, 1 - y), to_c).wait_recv()
        spread(12, j, block(1 - x, 1 - c, 1 - y), to_c).wait_recv()
        for g in range(8):
            y_ref[at(j), g * cols:(g + 1) * cols] = yall[g, at(j)].astype(y_ref.dtype)

    stages = ((finish_heads, 0), (finish_sum, 1), (multiply, 0), (forward, 2), (forward_last, 3), (emit, 4))
    for t in range(len(pieces) + 4):
        for stage, lag in stages:
            if 0 <= t - lag < len(pieces):
                stage(t - lag)
    for cp in pending:
        cp.wait_send()


def combine_and_project(parts_a, parts_b, w_o, hidden):
    ext, nb_a, head_dim = parts_a[0].shape
    nb_b = parts_b[0].shape[1]
    batch = nb_a + nb_b
    half = ext - 1
    heads = 2 * half
    cols = w_o.shape[1] // 8
    f32 = jnp.float32
    kinds, count = 13, B_PIECES + 1
    return pl.pallas_call(
        combine_kernel,
        out_shape=jax.ShapeDtypeStruct(hidden.shape, hidden.dtype),
        in_specs=[VMEM] * 6 + [ANY, ANY],
        out_specs=VMEM,
        scratch_shapes=[
            pltpu.VMEM((2, w_o.shape[0], cols), w_o.dtype),
            pltpu.VMEM((batch, cols), hidden.dtype),
            pltpu.VMEM((ext, nb_b, head_dim), f32),
            pltpu.VMEM((ext, nb_b, head_dim), f32),
            pltpu.VMEM((ext, nb_b, head_dim), f32),
            pltpu.VMEM((heads, batch, head_dim), f32),
            pltpu.VMEM((max(nb_a, nb_b // B_PIECES), heads * head_dim), jnp.bfloat16),
            pltpu.VMEM((2, batch, cols), f32),
            pltpu.VMEM((batch, cols), f32),
            pltpu.VMEM((8, batch, cols), f32),
            pltpu.SemaphoreType.DMA((3,)),
            pltpu.SemaphoreType.DMA((kinds, count)),
            pltpu.SemaphoreType.DMA((kinds, count)),
        ],
        compiler_params=pltpu.CompilerParams(collective_id=1, has_side_effects=True, vmem_limit_bytes=38 * 1024 * 1024),
        name='combine',
    )(*parts_a, *parts_b, w_o, hidden)


K_PIECES = 8
N_TILE = 1024
AHEAD = 5


def project_kernel(hid_hbm, gain_ref, len_ref, freq_ref, wq_hbm, wk_hbm, wv_hbm, q_ref, kv_ref, hid_ref, cos_ref, sin_ref, gain32, normed, acc, kv_acc, wbuf, kv_buf, hid_sem, w_sem, send, recv):
    batch, depth = hid_ref.shape
    head_dim = cos_ref.shape[1]
    q_cols = wq_hbm.shape[1] // 2
    kv_cols = wk_hbm.shape[1]
    k_rows = depth // K_PIECES
    q_tiles = q_cols // N_TILE
    sp = lax.axis_index('sp')
    c = lax.rem(sp, 2)
    to_c = {'sp': sp + 1 - 2 * c}

    barrier = pltpu.get_barrier_semaphore()
    pl.semaphore_signal(barrier, inc=1, device_id=to_c, device_id_type=MESH)

    def fetch(n, k):
        rows = pl.ds(k * k_rows, k_rows)
        if n == q_tiles:
            return tuple(pltpu.make_async_copy(src.at[rows], kv_buf.at[k], w_sem.at[n, k]) for src in (wk_hbm, wv_hbm))
        col = pl.ds(pl.multiple_of(c * q_cols + n * N_TILE, N_TILE), N_TILE)
        return (pltpu.make_async_copy(wq_hbm.at[rows, col], wbuf.at[n, k], w_sem.at[n, k]),)

    def start(n, k):
        cps = fetch(n, k)
        if n < q_tiles:
            cps[0].start()
            return
        for core in range(2):
            @pl.when(c == core)
            def _(core=core):
                cps[core].start()

    hid_copy = pltpu.make_async_copy(hid_hbm, hid_ref, hid_sem)
    hid_copy.start()
    order = [piece for k in range(K_PIECES) for piece in ((0, k), (q_tiles, k))]
    order += [(n, k) for n in range(1, q_tiles) for k in range(K_PIECES)]
    for piece in order[:AHEAD]:
        start(*piece)

    def angle_tables():
        angles = jnp.broadcast_to(len_ref[...].astype(jnp.float32), (batch, batch)).T[:, :head_dim] * jnp.concatenate([freq_ref[...]] * 2, axis=1)
        sin_ang = jnp.sin(angles)
        cos_ref[...] = jnp.cos(angles)
        sin_ref[...] = jnp.where(lax.broadcasted_iota(jnp.int32, angles.shape, 1) < head_dim // 2, -sin_ang, sin_ang)

    gain32[...] = gain_ref[...].astype(jnp.float32)
    hid_copy.wait()
    step = 1024
    total = jnp.zeros((batch, 1), jnp.float32)
    for j in range(depth // step):
        part = hid_ref[:, j * step:(j + 1) * step].astype(jnp.float32)
        total = total + jnp.sum(part * part, axis=-1, keepdims=True)
    inv_rms = lax.rsqrt(total / depth + NORM_EPS)
    lanes = gain_ref.shape[1]

    def normalize(k):
        for j in range(k * k_rows // lanes, (k + 1) * k_rows // lanes):
            sl = slice(j * lanes, (j + 1) * lanes)
            normed[:, sl] = (hid_ref[:, sl].astype(jnp.float32) * inv_rms * gain32[j:j + 1, :]).astype(normed.dtype)

    def round_bf16(v):
        return v.astype(jnp.bfloat16).astype(jnp.float32)

    def rope(v):
        return round_bf16(v * cos_ref[...] + pltpu.roll(v, head_dim // 2, 1) * sin_ref[...])

    sends = []

    def push(slot, ref, index):
        cp = pltpu.make_async_remote_copy(src_ref=ref.at[index], dst_ref=ref.at[index], send_sem=send.at[slot], recv_sem=recv.at[slot], device_id=to_c, device_id_type=MESH)
        if not sends:
            pl.semaphore_wait(barrier, 1)
        cp.start()
        sends.append(cp)

    per = N_TILE // head_dim

    def epilogue_kv():
        for h in range(kv_cols // head_dim):
            v = round_bf16(kv_acc[:, h * head_dim:(h + 1) * head_dim])
            kv_ref[c, :, h, :] = jnp.where(c == 0, rope(v), v)
        push(q_tiles, kv_ref, c)

    def epilogue(n):
        for h in range(per):
            q_ref[c, :, n * per + h, :] = rope(round_bf16(acc[n % 2, :, h * head_dim:(h + 1) * head_dim]))
        push(n, q_ref, (c, slice(None), pl.ds(n * per, per)))

    for i, (n, k) in enumerate(order):
        fetch(n, k)[0].wait()
        if i + AHEAD < len(order):
            start(*order[i + AHEAD])
        if n == 0:
            normalize(k)
        lhs = normed[:, k * k_rows:(k + 1) * k_rows]
        if n == q_tiles:
            prod = jnp.dot(lhs, kv_buf[k], preferred_element_type=jnp.float32)
            kv_acc[...] = prod + kv_acc[...] if k else prod
        else:
            prod = jnp.dot(lhs, wbuf[n, k], preferred_element_type=jnp.float32)
            acc[n % 2] = prod + acc[n % 2] if k else prod
        if (n, k) == (0, 3):
            angle_tables()
        if (n, k) == (1, 1):
            epilogue_kv()
        if 0 < n < q_tiles and k == 2:
            epilogue(n - 1)
    epilogue(q_tiles - 1)
    for cp in sends:
        cp.wait()


def project(hidden, lengths, norm_gain, w_q, w_k, w_v, inv_freq):
    batch, depth = hidden.shape
    head_dim = 2 * inv_freq.shape[0]
    q_heads = w_q.shape[1] // 2 // head_dim
    kv_heads = w_k.shape[1] // head_dim
    q_tiles = w_q.shape[1] // 2 // N_TILE
    return pl.pallas_call(
        project_kernel,
        out_shape=(jax.ShapeDtypeStruct((2, batch, q_heads, head_dim), jnp.float32), jax.ShapeDtypeStruct((2, batch, kv_heads, head_dim), jnp.float32)),
        in_specs=[ANY, VMEM, VMEM, VMEM, ANY, ANY, ANY],
        out_specs=(VMEM, VMEM),
        scratch_shapes=[
            pltpu.VMEM((batch, depth), hidden.dtype),
            pltpu.VMEM((batch, head_dim), jnp.float32),
            pltpu.VMEM((batch, head_dim), jnp.float32),
            pltpu.VMEM((depth // 128, 128), jnp.float32),
            pltpu.VMEM((batch, depth), jnp.bfloat16),
            pltpu.VMEM((2, batch, N_TILE), jnp.float32),
            pltpu.VMEM((batch, w_k.shape[1]), jnp.float32),
            pltpu.VMEM((q_tiles, K_PIECES, depth // K_PIECES, N_TILE), w_q.dtype),
            pltpu.VMEM((K_PIECES, depth // K_PIECES, w_k.shape[1]), w_k.dtype),
            pltpu.SemaphoreType.DMA,
            pltpu.SemaphoreType.DMA((q_tiles + 1, K_PIECES)),
            pltpu.SemaphoreType.DMA((q_tiles + 1,)),
            pltpu.SemaphoreType.DMA((q_tiles + 1,)),
        ],
        compiler_params=pltpu.CompilerParams(collective_id=0, has_side_effects=True, vmem_limit_bytes=53 * 1024 * 1024),
        name='project',
    )(hidden, norm_gain.reshape(depth // 128, 128), lengths.reshape(1, batch), inv_freq.reshape(1, head_dim // 2), w_q, w_k, w_v)


def device_step(hidden, lengths, k_cache, v_cache, norm_gain, w_q, w_k, w_v, w_o, inv_freq):
    batch, slots, kv_local, head_dim = k_cache.shape
    q_all, kv_all = project(hidden, lengths, norm_gain, w_q, w_k, w_v, inv_freq)
    flat = (batch, slots * kv_local, head_dim)
    shared = (lengths, q_all, kv_all, k_cache.reshape(flat), v_cache.reshape(flat))
    k_upd, v_upd, own_a, oth_a = write_and_attend(0, FIRST, *shared)
    swap = lambda array, flip: lax.ppermute(array, 'sp', [(s, s ^ flip) for s in range(4)])
    parts_a = (own_a, swap(oth_a, 1), swap(own_a, 2), swap(oth_a, 3))
    k_upd, v_upd, own_b, oth_b = write_and_attend(FIRST, batch - FIRST, *shared, written=(k_upd, v_upd))
    y_out = combine_and_project(parts_a, (own_b, oth_b), w_o, hidden)
    return y_out, k_upd.reshape(k_cache.shape), v_upd.reshape(v_cache.shape)


def solution(mesh):
    cache_spec = P('dp', 'sp', 'tp', None)
    in_specs = (P('dp', None), P('dp'), cache_spec, cache_spec, P(None), P(None, 'tp'), P(None, 'tp'), P(None, 'tp'), P('tp', None), P(None))
    out_specs = (P('dp', None), cache_spec, cache_spec)
    return jax.shard_map(device_step, mesh=mesh, in_specs=in_specs, out_specs=out_specs, check_vma=False)
```

```python
import functools

import jax
import jax.numpy as jnp
from jax import lax
from jax.experimental import pallas as pl
from jax.experimental.pallas import tpu as pltpu
from jax.sharding import PartitionSpec as P

NORM_EPS = 1e-5
NEG_BIG = -3.0e38
LOG2E = 1.4426950408889634
ANY = pl.BlockSpec(memory_space=pl.ANY)
HBM = pl.BlockSpec(memory_space=pltpu.HBM)
VMEM = pl.BlockSpec(memory_space=pltpu.VMEM)
SMEM = pl.BlockSpec(memory_space=pltpu.SMEM)


CHUNK = 8
PART = 4
NBUF = 5
LAG = 2


def attend_kernel(first, count, len_ref, q_hbm, kv_hbm, k_hbm, v_hbm, *refs):
    ko_hbm, vo_hbm, own_ref, oth_ref, q_ref, kv_ref, kbuf, vbuf, obuf, mbuf, lbuf, in_sem, out_sem, q_sem = refs[-14:]
    batch, rows, head_dim = k_hbm.shape
    kv_local = kv_ref.shape[2]
    heads = 2 * q_ref.shape[2]
    slots = rows // kv_local
    steps = count // CHUNK
    slot_start = lax.axis_index('sp') * slots

    def copies_in(i, part):
        b = lax.rem(i, NBUF)
        src = pl.ds(first + i * CHUNK + part * PART, PART)
        dst = pl.ds(part * PART, PART)
        return (pltpu.make_async_copy(k_hbm.at[src], kbuf.at[b, dst], in_sem.at[0, b, part]),
                pltpu.make_async_copy(v_hbm.at[src], vbuf.at[b, dst], in_sem.at[1, b, part]))

    def copies_out(i, part):
        b = lax.rem(i, NBUF)
        src = pl.ds(part * PART, PART)
        dst = pl.ds(first + i * CHUNK + part * PART, PART)
        return (pltpu.make_async_copy(kbuf.at[b, src], ko_hbm.at[dst], out_sem.at[0, b, part]),
                pltpu.make_async_copy(vbuf.at[b, src], vo_hbm.at[dst], out_sem.at[1, b, part]))

    parts = range(CHUNK // PART)
    small = (pltpu.make_async_copy(q_hbm.at[:, pl.ds(first, count)], q_ref, q_sem.at[0]), pltpu.make_async_copy(kv_hbm.at[:, pl.ds(first, count)], kv_ref, q_sem.at[1]))
    for cp in small:
        cp.start()
    for i in range(NBUF - LAG):
        for part in parts:
            for cp in copies_in(i, part):
                cp.start()

    col = lax.broadcasted_iota(jnp.int32, (heads, rows), 1)
    row = lax.broadcasted_iota(jnp.int32, (heads, rows), 0)
    head_ok = lax.rem(col, kv_local) == row // (heads // kv_local)
    tile_slot = lax.broadcasted_iota(jnp.int32, (16, head_dim), 0) // kv_local
    lane = lax.broadcasted_iota(jnp.int32, (heads, batch), 1)
    score_scale = head_dim ** -0.5 * LOG2E
    half = heads // 2
    core = lax.rem(lax.axis_index('sp'), 2)

    def store_token(i, s):
        buf = lax.rem(i, NBUF)
        b = first + i * CHUNK + s
        pos = len_ref[b] - slot_start
        own = (pos >= 0) & (pos < slots)
        safe = jnp.where(own, pos, 0)
        per_tile = 16 // kv_local
        base = pl.multiple_of(safe // per_tile * 16, 16)
        pick = (tile_slot == lax.rem(safe, per_tile)) & own
        for dst, which in ((kbuf, 0), (vbuf, 1)):
            new = jnp.concatenate([kv_ref[which, b - first]] * per_tile, axis=0)
            old = dst[buf, s, pl.ds(base, 16), :].astype(jnp.float32)
            dst[buf, s, pl.ds(base, 16), :] = jnp.where(pick, new, old).astype(jnp.bfloat16)

    def attend_pair(i, s, m_all, l_all):
        buf = lax.rem(i, NBUF)
        b0 = first + i * CHUNK + s
        b1 = b0 + 1
        limit0 = (len_ref[b0] - slot_start + 1) * kv_local
        limit1 = (len_ref[b1] - slot_start + 1) * kv_local
        q0 = jnp.concatenate([q_ref[0, b0 - first], q_ref[1, b0 - first]], axis=0).astype(jnp.bfloat16)
        q1 = jnp.concatenate([q_ref[0, b1 - first], q_ref[1, b1 - first]], axis=0).astype(jnp.bfloat16)
        zero = jnp.zeros_like(q0)
        q = jnp.concatenate([jnp.concatenate([q0, zero], axis=1), jnp.concatenate([zero, q1], axis=1)], axis=0)
        k = jnp.concatenate([kbuf[buf, s], kbuf[buf, s + 1]], axis=1)
        v = jnp.concatenate([vbuf[buf, s], vbuf[buf, s + 1]], axis=1)
        scores = lax.dot_general(q, k, (((1,), (1,)), ((), ())), preferred_element_type=jnp.float32)
        valid = jnp.concatenate([head_ok & (col < limit0), head_ok & (col < limit1)], axis=0)
        scores = jnp.where(valid, scores * score_scale, NEG_BIG)
        top = jnp.max(scores, axis=-1, keepdims=True)
        weights = jnp.where(valid, jnp.exp2(scores - top), 0.0)
        total = jnp.sum(weights, axis=-1, keepdims=True)
        out = jnp.dot(weights.astype(jnp.bfloat16), v, preferred_element_type=jnp.float32)
        obuf[s] = out[:heads, :head_dim]
        obuf[s + 1] = out[heads:, head_dim:]
        m_all = jnp.where(lane == b0, top[:heads], jnp.where(lane == b1, top[heads:], m_all))
        l_all = jnp.where(lane == b0, total[:heads], jnp.where(lane == b1, total[heads:], l_all))
        return m_all, l_all

    def step(i, carry):
        for part in parts:
            @pl.when((i >= LAG) & (i + NBUF - LAG < steps))
            def _():
                for cp in copies_out(i - LAG, part):
                    cp.wait()

            @pl.when(i + NBUF - LAG < steps)
            def _():
                for cp in copies_in(i + NBUF - LAG, part):
                    cp.start()

        m_all, l_all = mbuf[...], lbuf[...]
        for part in parts:
            for cp in copies_in(i, part):
                cp.wait()
            for s in range(part * PART, (part + 1) * PART):
                store_token(i, s)
            for s in range(part * PART, (part + 1) * PART, 2):
                m_all, l_all = attend_pair(i, s, m_all, l_all)
            for cp in copies_out(i, part):
                cp.start()
        mbuf[...] = m_all
        lbuf[...] = l_all
        out_rows = pl.ds(pl.multiple_of(i * CHUNK, CHUNK), CHUNK)
        by_head = jnp.swapaxes(obuf[...], 0, 1)
        own_ref[:half, out_rows] = jnp.where(core == 0, by_head[:half], by_head[half:])
        oth_ref[:half, out_rows] = jnp.where(core == 0, by_head[half:], by_head[:half])

        return carry

    mbuf[...] = jnp.zeros_like(mbuf)
    lbuf[...] = jnp.zeros_like(lbuf)
    for cp in small:
        cp.wait()
    lax.fori_loop(0, steps, step, 0)
    for i in range(steps - NBUF, steps):
        for part in parts:
            for cp in copies_out(i, part):
                cp.wait()
    stats = []
    for lo in (0, half):
        rows_ml = [mbuf[lo:lo + half], lbuf[lo:lo + half], jnp.zeros((batch - 2 * half, batch), jnp.float32)]
        stats.append(jnp.concatenate(rows_ml, axis=0).T[first:first + count])
    own_ref[half] = jnp.where(core == 0, stats[0], stats[1])
    oth_ref[half] = jnp.where(core == 0, stats[1], stats[0])


def write_and_attend(first, count, lengths, q_all, kv_all, k_cache, v_cache, written=()):
    batch, rows, head_dim = k_cache.shape
    heads = q_all.shape[0] * q_all.shape[2]
    part = jax.ShapeDtypeStruct((heads // 2 + 1, count, head_dim), jnp.float32)
    cache = jax.ShapeDtypeStruct(k_cache.shape, k_cache.dtype)
    return pl.pallas_call(
        functools.partial(attend_kernel, first, count),
        out_shape=(cache, cache, part, part),
        in_specs=[SMEM] + [HBM] * 4 + [ANY] * len(written),
        out_specs=(ANY, ANY, VMEM, VMEM),
        input_output_aliases={5: 0, 6: 1} if written else {},
        scratch_shapes=[
            pltpu.VMEM((2, count) + q_all.shape[2:], jnp.float32),
            pltpu.VMEM((2, count) + kv_all.shape[2:], jnp.float32),
            pltpu.VMEM((NBUF, CHUNK, rows, head_dim), jnp.bfloat16),
            pltpu.VMEM((NBUF, CHUNK, rows, head_dim), jnp.bfloat16),
            pltpu.VMEM((CHUNK, heads, head_dim), jnp.float32),
            pltpu.VMEM((heads, batch), jnp.float32),
            pltpu.VMEM((heads, batch), jnp.float32),
            pltpu.SemaphoreType.DMA((2, NBUF, CHUNK // PART)),
            pltpu.SemaphoreType.DMA((2, NBUF, CHUNK // PART)),
            pltpu.SemaphoreType.DMA((2,)),
        ],
        compiler_params=pltpu.CompilerParams(vmem_limit_bytes=34 * 1024 * 1024),
        cost_estimate=pl.CostEstimate(flops=100 * count * heads * rows * head_dim, bytes_accessed=8 * count * rows * head_dim, transcendentals=0),
        name='attend',
    )(lengths, q_all, kv_all, k_cache, v_cache, *written)


FIRST = 64
PIECES = (64, 48, 16)
MODES = 'QPD'
LAGS = (0, 1, 0, 2, 3, 4)
MESH = pl.DeviceIdType.MESH


def weigh(tiles):
    half = 16
    tops = [t[:, :half] for t in tiles]
    top = functools.reduce(jnp.maximum, tops)
    scales = [jnp.exp2(m - top) for m in tops]
    total = sum(t[:, half:2 * half] * s for t, s in zip(tiles, scales))
    return top, total, scales


def combine_kernel(own_a, core_a, x_a, diag_a, own_b, oth_b, w_hbm, hid_hbm, y_ref, w, hid, r1, c1, r2, att, lhs, part, r3, yall,
                   w_sem, send, recv):
    heads, batch, head_dim = att.shape
    half = heads // 2
    cols = part.shape[2]
    first = own_a.shape[1]
    pieces = [(sum(PIECES[:j]), n) for j, n in enumerate(PIECES)]
    count = len(pieces)
    sp, y = lax.axis_index('sp'), lax.axis_index('tp')
    c, x = lax.rem(sp, 2), sp // 2
    to_c, to_x, to_y = {'sp': sp + 1 - 2 * c}, {'sp': sp + 2 - 4 * x}, {'tp': 1 - y}
    block = lambda xx, cc, yy: 4 * xx + 2 * cc + yy
    mine = block(x, c, y)

    barrier = pltpu.get_barrier_semaphore()
    for dev in (to_c, to_x, to_y):
        pl.semaphore_signal(barrier, inc=1, device_id=dev, device_id_type=MESH)

    w_copies = [pltpu.make_async_copy(w_hbm.at[:, pl.ds(pl.multiple_of((2 * sp + h) * cols, cols), cols)], w.at[h], w_sem.at[h]) for h in range(2)]
    w_copies += [pltpu.make_async_copy(hid_hbm.at[:, pl.ds(pl.multiple_of((2 * sp + h) * cols, cols), cols)], hid.at[h], w_sem.at[2 + h]) for h in range(2)]
    for cp in w_copies:
        cp.start()
    pl.semaphore_wait(barrier, 3)

    def copy(kind, j, src, dst, dev):
        return pltpu.make_async_remote_copy(src_ref=src, dst_ref=dst, send_sem=send.at[kind, j], recv_sem=recv.at[kind, j], device_id=dev, device_id_type=MESH)

    def at(j):
        return pl.ds(*pieces[j])

    def local(j):
        return pl.ds(pieces[j][0] - first, pieces[j][1])

    pending = []

    def push(cp):
        cp.start()
        pending.append(cp)

    b_range = range(1, count)
    stat_c = copy(0, 0, oth_b.at[half], r1.at[half], to_c)
    push(stat_c)
    o_copies = {j: copy(1, j, oth_b.at[pl.ds(0, half), local(j)], r1.at[pl.ds(0, half), local(j)], to_c) for j in b_range}
    for j in b_range:
        push(o_copies[j])

    own_att = att.at[pl.ds(c * half, half)]
    att_copies = [copy(4, j, own_att.at[:, at(j)], own_att.at[:, at(j)], to_c) for j in range(count)]
    part_copies = [copy(5, j, part.at[1 - y, at(j)], r3.at[1 - y, at(j)], to_y) for j in range(count)]

    parts_a = (own_a, core_a, x_a, diag_a)
    _, total, scales = weigh([p[half] for p in parts_a])
    scales = [s / total for s in scales]
    for h in range(half):
        att[c * half + h, at(0)] = sum(p[h] * s[:, h:h + 1] for p, s in zip(parts_a, scales))
    push(att_copies[0])

    stat_c.wait_recv()
    top, total, scales = weigh([own_b[half], r1[half]])
    c1[half] = jnp.concatenate([top, total, jnp.zeros((own_b.shape[1], head_dim - 2 * half), jnp.float32)], axis=1)
    stat_x = copy(2, 0, c1.at[half], r2.at[half], to_x)
    push(stat_x)
    x_copies = {j: copy(3, j, c1.at[pl.ds(0, half), local(j)], r2.at[pl.ds(0, half), local(j)], to_x) for j in b_range}
    for j in b_range:
        o_copies[j].wait_recv()
        lo, n = pieces[j][0] - first, pieces[j][1]
        for h in range(half):
            c1[h, local(j)] = own_b[h, local(j)] * scales[0][lo:lo + n, h:h + 1] + r1[h, local(j)] * scales[1][lo:lo + n, h:h + 1]
        push(x_copies[j])

    def spread(kind, j, blk, dev):
        return copy(kind, j, yall.at[blk, at(j)], yall.at[blk, at(j)], dev)

    b_x, b_y, b_xy = block(1 - x, c, y), block(x, c, 1 - y), block(1 - x, c, 1 - y)
    final = {}

    def finish_heads(j):
        if j == 0:
            return
        if j == 1:
            stat_x.wait_recv()
            _, tot, sc = weigh([c1[half], r2[half]])
            final['scales'] = [s / tot for s in sc]
        x_copies[j].wait_recv()
        lo, n = pieces[j][0] - first, pieces[j][1]
        for h in range(half):
            att[c * half + h, at(j)] = sum(p[h, local(j)] * s[lo:lo + n, h:h + 1] for p, s in zip((c1, r2), final['scales']))
        push(att_copies[j])

    def multiply(j):
        if j == 0:
            for cp in w_copies:
                cp.wait()
        att_copies[j].wait_recv()
        n = pieces[j][1]
        for h in range(heads):
            lhs[:n, h * head_dim:(h + 1) * head_dim] = att[h, at(j)].astype(jnp.bfloat16)

        def tiles(side):
            def tile(i, carry):
                sl = pl.ds(pl.multiple_of(i * 256, 256), 256)
                part[side, at(j), sl] = jnp.dot(lhs[:n], w[side, :, sl], preferred_element_type=jnp.float32)
                return carry
            lax.fori_loop(0, cols // 256, tile, 0)

        tiles(1 - y)
        push(part_copies[j])
        tiles(y)
        if MODES[j] == 'D':
            push(both_copy(j))

    def both_copy(j):
        return copy(13, j, part.at[y, at(j)], r3.at[y, at(j)], to_y)

    def finish_sum(j):
        part_copies[j].wait_recv()
        if MODES[j] == 'D':
            both_copy(j).wait_recv()
            for side in range(2):
                yall[block(x, c, side), at(j)] = hid[side, at(j)].astype(jnp.float32) + (part[side, at(j)] + r3[side, at(j)])
            push(spread(7, j, mine, to_x))
            push(spread(10, j, b_y, to_x))
            push(spread(6, j, mine, to_c))
            push(spread(11, j, b_y, to_c))
            return
        yall[mine, at(j)] = hid[y, at(j)].astype(jnp.float32) + (part[y, at(j)] + r3[y, at(j)])
        push(spread(8, j, mine, to_y))
        push(spread(7, j, mine, to_x))
        push(spread(6, j, mine, to_c))

    def forward(j):
        def from_x():
            spread(7, j, b_x, to_x).wait_recv()
            if MODES[j] == 'P':
                push(spread(10, j, b_x, to_y))
            push(spread(9, j, b_x, to_c))

        def from_y():
            spread(8, j, b_y, to_y).wait_recv()
            if MODES[j] == 'Q':
                push(spread(10, j, b_y, to_x))
            push(spread(11, j, b_y, to_c))

        for take in {'P': (from_x, from_y), 'Q': (from_y, from_x), 'D': (from_x,)}[MODES[j]]:
            take()

    def forward_last(j):
        spread(10, j, b_xy, to_y).wait_recv()
        push(spread(12, j, b_xy, to_c))

    def emit(j):
        spread(6, j, block(x, 1 - c, y), to_c).wait_recv()
        spread(9, j, block(1 - x, 1 - c, y), to_c).wait_recv()
        spread(11, j, block(x, 1 - c, 1 - y), to_c).wait_recv()
        spread(12, j, block(1 - x, 1 - c, 1 - y), to_c).wait_recv()
        for g in range(8):
            y_ref[at(j), g * cols:(g + 1) * cols] = yall[g, at(j)].astype(y_ref.dtype)

    stages = tuple(zip((finish_heads, finish_sum, multiply, forward, forward_last, emit), LAGS))
    for t in range(count + max(LAGS)):
        for stage, lag in stages:
            if 0 <= t - lag < count:
                stage(t - lag)
    for cp in pending:
        cp.wait_send()


def combine_and_project(parts_a, parts_b, w_o, hidden):
    ext, nb_a, head_dim = parts_a[0].shape
    nb_b = parts_b[0].shape[1]
    batch = nb_a + nb_b
    half = ext - 1
    heads = 2 * half
    cols = w_o.shape[1] // 8
    f32 = jnp.float32
    kinds, count = 14, len(PIECES)
    return pl.pallas_call(
        combine_kernel,
        out_shape=jax.ShapeDtypeStruct(hidden.shape, hidden.dtype),
        in_specs=[VMEM] * 6 + [ANY, ANY],
        out_specs=VMEM,
        scratch_shapes=[
            pltpu.VMEM((2, w_o.shape[0], cols), w_o.dtype),
            pltpu.VMEM((2, batch, cols), hidden.dtype),
            pltpu.VMEM((ext, nb_b, head_dim), f32),
            pltpu.VMEM((ext, nb_b, head_dim), f32),
            pltpu.VMEM((ext, nb_b, head_dim), f32),
            pltpu.VMEM((heads, batch, head_dim), f32),
            pltpu.VMEM((max(PIECES), heads * head_dim), jnp.bfloat16),
            pltpu.VMEM((2, batch, cols), f32),
            pltpu.VMEM((2, batch, cols), f32),
            pltpu.VMEM((8, batch, cols), f32),
            pltpu.SemaphoreType.DMA((4,)),
            pltpu.SemaphoreType.DMA((kinds, count)),
            pltpu.SemaphoreType.DMA((kinds, count)),
        ],
        compiler_params=pltpu.CompilerParams(collective_id=1, has_side_effects=True, vmem_limit_bytes=38 * 1024 * 1024),
        name='combine',
    )(*parts_a, *parts_b, w_o, hidden)


K_PIECES = 8
N_TILE = 1024
AHEAD = 8


def project_kernel(hid_hbm, gain_hbm, len_hbm, freq_hbm, wq_hbm, wk_hbm, wv_hbm, q_ref, kv_ref, hid_ref, gain_ref, len_ref, freq_ref, cos_ref, sin_ref, gain32, normed, acc, kv_acc, wbuf, kv_buf, hid_sem, w_sem, send, recv):
    batch, depth = hid_ref.shape
    head_dim = cos_ref.shape[1]
    q_cols = wq_hbm.shape[1] // 2
    kv_cols = wk_hbm.shape[1]
    k_rows = depth // K_PIECES
    q_tiles = q_cols // N_TILE
    sp = lax.axis_index('sp')
    c = lax.rem(sp, 2)
    to_c = {'sp': sp + 1 - 2 * c}

    barrier = pltpu.get_barrier_semaphore()
    pl.semaphore_signal(barrier, inc=1, device_id=to_c, device_id_type=MESH)

    def fetch(n, k):
        rows = pl.ds(k * k_rows, k_rows)
        if n == q_tiles:
            return tuple(pltpu.make_async_copy(src.at[rows], kv_buf.at[k], w_sem.at[n, k]) for src in (wk_hbm, wv_hbm))
        col = pl.ds(pl.multiple_of(c * q_cols + n * N_TILE, N_TILE), N_TILE)
        return (pltpu.make_async_copy(wq_hbm.at[rows, col], wbuf.at[n, k], w_sem.at[n, k]),)

    def start(n, k):
        cps = fetch(n, k)
        if n < q_tiles:
            cps[0].start()
            return
        for core in range(2):
            @pl.when(c == core)
            def _(core=core):
                cps[core].start()

    small = [pltpu.make_async_copy(src, dst, hid_sem.at[i]) for i, (src, dst) in enumerate(
        ((hid_hbm, hid_ref), (gain_hbm, gain_ref), (len_hbm, len_ref), (freq_hbm, freq_ref)))]
    for cp in small:
        cp.start()
    order = [piece for k in range(K_PIECES) for piece in ((0, k), (q_tiles, k))]
    order += [(n, k) for n in range(1, q_tiles) for k in range(K_PIECES)]
    for piece in order[:AHEAD]:
        start(*piece)

    def angle_tables():
        angles = jnp.broadcast_to(len_ref[...].astype(jnp.float32), (batch, batch)).T[:, :head_dim] * jnp.concatenate([freq_ref[...]] * 2, axis=1)
        sin_ang = jnp.sin(angles)
        cos_ref[...] = jnp.cos(angles)
        sin_ref[...] = jnp.where(lax.broadcasted_iota(jnp.int32, angles.shape, 1) < head_dim // 2, -sin_ang, sin_ang)

    for cp in small:
        cp.wait()
    gain32[...] = gain_ref[...].astype(jnp.float32)
    step = 1024
    total = jnp.zeros((batch, 1), jnp.float32)
    for j in range(depth // step):
        part = hid_ref[:, j * step:(j + 1) * step].astype(jnp.float32)
        total = total + jnp.sum(part * part, axis=-1, keepdims=True)
    inv_rms = lax.rsqrt(total / depth + NORM_EPS)
    lanes = gain_ref.shape[1]

    def normalize(k):
        for j in range(k * k_rows // lanes, (k + 1) * k_rows // lanes):
            sl = slice(j * lanes, (j + 1) * lanes)
            normed[:, sl] = (hid_ref[:, sl].astype(jnp.float32) * inv_rms * gain32[j:j + 1, :]).astype(normed.dtype)

    def round_bf16(v):
        return v.astype(jnp.bfloat16).astype(jnp.float32)

    def rope(v):
        return round_bf16(v * cos_ref[...] + pltpu.roll(v, head_dim // 2, 1) * sin_ref[...])

    sends = []

    def push(slot, ref, index):
        cp = pltpu.make_async_remote_copy(src_ref=ref.at[index], dst_ref=ref.at[index], send_sem=send.at[slot], recv_sem=recv.at[slot], device_id=to_c, device_id_type=MESH)
        if not sends:
            pl.semaphore_wait(barrier, 1)
        cp.start()
        sends.append(cp)

    per = N_TILE // head_dim

    def epilogue_kv():
        for h in range(kv_cols // head_dim):
            v = round_bf16(kv_acc[:, h * head_dim:(h + 1) * head_dim])
            kv_ref[c, :, h, :] = jnp.where(c == 0, rope(v), v)
        push(q_tiles, kv_ref, c)

    def epilogue(n):
        for h in range(per):
            q_ref[c, :, n * per + h, :] = rope(round_bf16(acc[n % 2, :, h * head_dim:(h + 1) * head_dim]))
        push(n, q_ref, (c, slice(None), pl.ds(n * per, per)))

    for i, (n, k) in enumerate(order):
        fetch(n, k)[0].wait()
        if i + AHEAD < len(order):
            start(*order[i + AHEAD])
        if n == 0:
            normalize(k)
        lhs = normed[:, k * k_rows:(k + 1) * k_rows]
        if n == q_tiles:
            prod = jnp.dot(lhs, kv_buf[k], preferred_element_type=jnp.float32)
            kv_acc[...] = prod + kv_acc[...] if k else prod
        else:
            prod = jnp.dot(lhs, wbuf[n, k], preferred_element_type=jnp.float32)
            acc[n % 2] = prod + acc[n % 2] if k else prod
        if (n, k) == (0, 3):
            angle_tables()
        if (n, k) == (1, 1):
            epilogue_kv()
        if 0 < n < q_tiles and k == 2:
            epilogue(n - 1)
    epilogue(q_tiles - 1)
    for cp in sends:
        cp.wait()


def project(hidden, lengths, norm_gain, w_q, w_k, w_v, inv_freq):
    batch, depth = hidden.shape
    head_dim = 2 * inv_freq.shape[0]
    q_heads = w_q.shape[1] // 2 // head_dim
    kv_heads = w_k.shape[1] // head_dim
    q_tiles = w_q.shape[1] // 2 // N_TILE
    return pl.pallas_call(
        project_kernel,
        out_shape=(jax.ShapeDtypeStruct((2, batch, q_heads, head_dim), jnp.float32), jax.ShapeDtypeStruct((2, batch, kv_heads, head_dim), jnp.float32)),
        in_specs=[HBM] * 7,
        out_specs=(VMEM, VMEM),
        scratch_shapes=[
            pltpu.VMEM((batch, depth), hidden.dtype),
            pltpu.VMEM((depth // 128, 128), norm_gain.dtype),
            pltpu.VMEM((1, batch), jnp.int32),
            pltpu.VMEM((1, head_dim // 2), jnp.float32),
            pltpu.VMEM((batch, head_dim), jnp.float32),
            pltpu.VMEM((batch, head_dim), jnp.float32),
            pltpu.VMEM((depth // 128, 128), jnp.float32),
            pltpu.VMEM((batch, depth), jnp.bfloat16),
            pltpu.VMEM((2, batch, N_TILE), jnp.float32),
            pltpu.VMEM((batch, w_k.shape[1]), jnp.float32),
            pltpu.VMEM((q_tiles, K_PIECES, depth // K_PIECES, N_TILE), w_q.dtype),
            pltpu.VMEM((K_PIECES, depth // K_PIECES, w_k.shape[1]), w_k.dtype),
            pltpu.SemaphoreType.DMA((4,)),
            pltpu.SemaphoreType.DMA((q_tiles + 1, K_PIECES)),
            pltpu.SemaphoreType.DMA((q_tiles + 1,)),
            pltpu.SemaphoreType.DMA((q_tiles + 1,)),
        ],
        compiler_params=pltpu.CompilerParams(collective_id=0, has_side_effects=True, vmem_limit_bytes=50 * 1024 * 1024),
        name='project',
    )(hidden, norm_gain.reshape(depth // 128, 128), lengths.reshape(1, batch), inv_freq.reshape(1, head_dim // 2), w_q, w_k, w_v)


def device_step(hidden, lengths, k_cache, v_cache, norm_gain, w_q, w_k, w_v, w_o, inv_freq):
    batch, slots, kv_local, head_dim = k_cache.shape
    q_all, kv_all = project(hidden, lengths, norm_gain, w_q, w_k, w_v, inv_freq)
    flat = (batch, slots * kv_local, head_dim)
    shared = (lengths, q_all, kv_all, k_cache.reshape(flat), v_cache.reshape(flat))
    k_upd, v_upd, own_a, oth_a = write_and_attend(0, FIRST, *shared)
    swap = lambda array, flip: lax.ppermute(array, 'sp', [(s, s ^ flip) for s in range(4)])
    parts_a = (own_a, swap(oth_a, 1), swap(own_a, 2), swap(oth_a, 3))
    k_upd, v_upd, own_b, oth_b = write_and_attend(FIRST, batch - FIRST, *shared, written=(k_upd, v_upd))
    y_out = combine_and_project(parts_a, (own_b, oth_b), w_o, hidden)
    return y_out, k_upd.reshape(k_cache.shape), v_upd.reshape(v_cache.shape)


def solution(mesh):
    cache_spec = P('dp', 'sp', 'tp', None)
    in_specs = (P('dp', None), P('dp'), cache_spec, cache_spec, P(None), P(None, 'tp'), P(None, 'tp'), P(None, 'tp'), P('tp', None), P(None))
    out_specs = (P('dp', None), cache_spec, cache_spec)
    return jax.shard_map(device_step, mesh=mesh, in_specs=in_specs, out_specs=out_specs, check_vma=False)
```

```python
import functools

import jax
import jax.numpy as jnp
from jax import lax
from jax.experimental import pallas as pl
from jax.experimental.pallas import tpu as pltpu
from jax.sharding import PartitionSpec as P

NORM_EPS = 1e-5
NEG_BIG = -3.0e38
LOG2E = 1.4426950408889634
ANY = pl.BlockSpec(memory_space=pl.ANY)
HBM = pl.BlockSpec(memory_space=pltpu.HBM)
VMEM = pl.BlockSpec(memory_space=pltpu.VMEM)
SMEM = pl.BlockSpec(memory_space=pltpu.SMEM)


CHUNK = 8
PART = 4
NBUF = 5
LAG = 2


def attend_kernel(first, count, len_ref, q_hbm, kv_hbm, k_hbm, v_hbm, *refs):
    ko_hbm, vo_hbm, own_ref, oth_ref, q_ref, kv_ref, kbuf, vbuf, obuf, mbuf, lbuf, in_sem, out_sem, q_sem = refs[-14:]
    batch, rows, head_dim = k_hbm.shape
    kv_local = kv_ref.shape[2]
    heads = 2 * q_ref.shape[2]
    slots = rows // kv_local
    steps = count // CHUNK
    slot_start = lax.axis_index('sp') * slots

    def copies_in(i, part):
        b = lax.rem(i, NBUF)
        src = pl.ds(first + i * CHUNK + part * PART, PART)
        dst = pl.ds(part * PART, PART)
        return (pltpu.make_async_copy(k_hbm.at[src], kbuf.at[b, dst], in_sem.at[0, b, part]),
                pltpu.make_async_copy(v_hbm.at[src], vbuf.at[b, dst], in_sem.at[1, b, part]))

    def copies_out(i, part):
        b = lax.rem(i, NBUF)
        src = pl.ds(part * PART, PART)
        dst = pl.ds(first + i * CHUNK + part * PART, PART)
        return (pltpu.make_async_copy(kbuf.at[b, src], ko_hbm.at[dst], out_sem.at[0, b, part]),
                pltpu.make_async_copy(vbuf.at[b, src], vo_hbm.at[dst], out_sem.at[1, b, part]))

    parts = range(CHUNK // PART)
    small = (pltpu.make_async_copy(q_hbm.at[:, pl.ds(first, count)], q_ref, q_sem.at[0]), pltpu.make_async_copy(kv_hbm.at[:, pl.ds(first, count)], kv_ref, q_sem.at[1]))
    for cp in small:
        cp.start()
    for i in range(NBUF - LAG):
        for part in parts:
            for cp in copies_in(i, part):
                cp.start()

    col = lax.broadcasted_iota(jnp.int32, (heads, rows), 1)
    row = lax.broadcasted_iota(jnp.int32, (heads, rows), 0)
    head_ok = lax.rem(col, kv_local) == row // (heads // kv_local)
    tile_slot = lax.broadcasted_iota(jnp.int32, (16, head_dim), 0) // kv_local
    lane = lax.broadcasted_iota(jnp.int32, (heads, batch), 1)
    score_scale = head_dim ** -0.5 * LOG2E
    half = heads // 2
    core = lax.rem(lax.axis_index('sp'), 2)

    def store_token(i, s):
        buf = lax.rem(i, NBUF)
        b = first + i * CHUNK + s
        pos = len_ref[b] - slot_start
        own = (pos >= 0) & (pos < slots)
        safe = jnp.where(own, pos, 0)
        per_tile = 16 // kv_local
        base = pl.multiple_of(safe // per_tile * 16, 16)
        pick = (tile_slot == lax.rem(safe, per_tile)) & own
        for dst, which in ((kbuf, 0), (vbuf, 1)):
            new = jnp.concatenate([kv_ref[which, b - first]] * per_tile, axis=0)
            old = dst[buf, s, pl.ds(base, 16), :].astype(jnp.float32)
            dst[buf, s, pl.ds(base, 16), :] = jnp.where(pick, new, old).astype(jnp.bfloat16)

    def attend_pair(i, s, m_all, l_all):
        buf = lax.rem(i, NBUF)
        b0 = first + i * CHUNK + s
        b1 = b0 + 1
        limit0 = (len_ref[b0] - slot_start + 1) * kv_local
        limit1 = (len_ref[b1] - slot_start + 1) * kv_local
        q0 = jnp.concatenate([q_ref[0, b0 - first], q_ref[1, b0 - first]], axis=0).astype(jnp.bfloat16)
        q1 = jnp.concatenate([q_ref[0, b1 - first], q_ref[1, b1 - first]], axis=0).astype(jnp.bfloat16)
        zero = jnp.zeros_like(q0)
        q = jnp.concatenate([jnp.concatenate([q0, zero], axis=1), jnp.concatenate([zero, q1], axis=1)], axis=0)
        k = jnp.concatenate([kbuf[buf, s], kbuf[buf, s + 1]], axis=1)
        v = jnp.concatenate([vbuf[buf, s], vbuf[buf, s + 1]], axis=1)
        scores = lax.dot_general(q, k, (((1,), (1,)), ((), ())), preferred_element_type=jnp.float32)
        valid = jnp.concatenate([head_ok & (col < limit0), head_ok & (col < limit1)], axis=0)
        scores = jnp.where(valid, scores * score_scale, NEG_BIG)
        top = jnp.max(scores, axis=-1, keepdims=True)
        weights = jnp.where(valid, jnp.exp2(scores - top), 0.0)
        total = jnp.sum(weights, axis=-1, keepdims=True)
        out = jnp.dot(weights.astype(jnp.bfloat16), v, preferred_element_type=jnp.float32)
        obuf[s] = out[:heads, :head_dim]
        obuf[s + 1] = out[heads:, head_dim:]
        m_all = jnp.where(lane == b0, top[:heads], jnp.where(lane == b1, top[heads:], m_all))
        l_all = jnp.where(lane == b0, total[:heads], jnp.where(lane == b1, total[heads:], l_all))
        return m_all, l_all

    def step(i, carry):
        for part in parts:
            @pl.when((i >= LAG) & (i + NBUF - LAG < steps))
            def _():
                for cp in copies_out(i - LAG, part):
                    cp.wait()

            @pl.when(i + NBUF - LAG < steps)
            def _():
                for cp in copies_in(i + NBUF - LAG, part):
                    cp.start()

        m_all, l_all = mbuf[...], lbuf[...]
        for part in parts:
            for cp in copies_in(i, part):
                cp.wait()
            for s in range(part * PART, (part + 1) * PART):
                store_token(i, s)
            for s in range(part * PART, (part + 1) * PART, 2):
                m_all, l_all = attend_pair(i, s, m_all, l_all)
            for cp in copies_out(i, part):
                cp.start()
        mbuf[...] = m_all
        lbuf[...] = l_all
        out_rows = pl.ds(pl.multiple_of(i * CHUNK, CHUNK), CHUNK)
        by_head = jnp.swapaxes(obuf[...], 0, 1)
        own_ref[:half, out_rows] = jnp.where(core == 0, by_head[:half], by_head[half:])
        oth_ref[:half, out_rows] = jnp.where(core == 0, by_head[half:], by_head[:half])

        return carry

    mbuf[...] = jnp.zeros_like(mbuf)
    lbuf[...] = jnp.zeros_like(lbuf)
    for cp in small:
        cp.wait()
    lax.fori_loop(0, steps, step, 0)
    for i in range(steps - NBUF, steps):
        for part in parts:
            for cp in copies_out(i, part):
                cp.wait()
    stats = []
    for lo in (0, half):
        rows_ml = [mbuf[lo:lo + half], lbuf[lo:lo + half], jnp.zeros((batch - 2 * half, batch), jnp.float32)]
        stats.append(jnp.concatenate(rows_ml, axis=0).T[first:first + count])
    own_ref[half] = jnp.where(core == 0, stats[0], stats[1])
    oth_ref[half] = jnp.where(core == 0, stats[1], stats[0])


def write_and_attend(first, count, lengths, q_all, kv_all, k_cache, v_cache, written=()):
    batch, rows, head_dim = k_cache.shape
    heads = q_all.shape[0] * q_all.shape[2]
    part = jax.ShapeDtypeStruct((heads // 2 + 1, count, head_dim), jnp.float32)
    cache = jax.ShapeDtypeStruct(k_cache.shape, k_cache.dtype)
    return pl.pallas_call(
        functools.partial(attend_kernel, first, count),
        out_shape=(cache, cache, part, part),
        in_specs=[SMEM] + [HBM] * 4 + [ANY] * len(written),
        out_specs=(ANY, ANY, VMEM, VMEM),
        input_output_aliases={5: 0, 6: 1} if written else {},
        scratch_shapes=[
            pltpu.VMEM((2, count) + q_all.shape[2:], jnp.float32),
            pltpu.VMEM((2, count) + kv_all.shape[2:], jnp.float32),
            pltpu.VMEM((NBUF, CHUNK, rows, head_dim), jnp.bfloat16),
            pltpu.VMEM((NBUF, CHUNK, rows, head_dim), jnp.bfloat16),
            pltpu.VMEM((CHUNK, heads, head_dim), jnp.float32),
            pltpu.VMEM((heads, batch), jnp.float32),
            pltpu.VMEM((heads, batch), jnp.float32),
            pltpu.SemaphoreType.DMA((2, NBUF, CHUNK // PART)),
            pltpu.SemaphoreType.DMA((2, NBUF, CHUNK // PART)),
            pltpu.SemaphoreType.DMA((2,)),
        ],
        compiler_params=pltpu.CompilerParams(vmem_limit_bytes=34 * 1024 * 1024),
        cost_estimate=pl.CostEstimate(flops=100 * count * heads * rows * head_dim, bytes_accessed=8 * count * rows * head_dim, transcendentals=0),
        name='attend',
    )(lengths, q_all, kv_all, k_cache, v_cache, *written)


FIRST = 64
PIECES = (64, 48, 16)
UNITS = ((0, 32, 'Q'), (0, 32, 'Q'), (1, 24, 'P'), (1, 24, 'P'), (2, 16, 'D'))
ORDER = 'm0 s0 s1 h1 m1 h2 f0 f1 s2 m2 s3 f2 s4 f3 f4 l0 l1 l2 l3 l4 e0 e1 e2 e3 e4'
MESH = pl.DeviceIdType.MESH


def weigh(tiles):
    half = 16
    tops = [t[:, :half] for t in tiles]
    top = functools.reduce(jnp.maximum, tops)
    scales = [jnp.exp2(m - top) for m in tops]
    total = sum(t[:, half:2 * half] * s for t, s in zip(tiles, scales))
    return top, total, scales


def combine_kernel(own_a, core_a, x_a, diag_a, own_b, oth_b, w_hbm, hid_hbm, y_ref, w, hid, r1, c1, r2, att, lhs, part, r3, yall,
                   w_sem, send, recv):
    heads, batch, head_dim = att.shape
    half = heads // 2
    cols = part.shape[2]
    first = own_a.shape[1]
    pieces = [(sum(PIECES[:j]), n) for j, n in enumerate(PIECES)]
    count = len(pieces)
    units = [(sum(n for _, n, _ in UNITS[:u]), n) for u, (_, n, _) in enumerate(UNITS)]
    units_of = [[u for u, unit in enumerate(UNITS) if unit[0] == j] for j in range(count)]
    direct = [UNITS[us[0]][2] == 'D' for us in units_of]
    sp, y = lax.axis_index('sp'), lax.axis_index('tp')
    c, x = lax.rem(sp, 2), sp // 2
    to_c, to_x, to_y = {'sp': sp + 1 - 2 * c}, {'sp': sp + 2 - 4 * x}, {'tp': 1 - y}
    block = lambda xx, cc, yy: 4 * xx + 2 * cc + yy
    mine = block(x, c, y)

    barrier = pltpu.get_barrier_semaphore()
    for dev in (to_c, to_x, to_y):
        pl.semaphore_signal(barrier, inc=1, device_id=dev, device_id_type=MESH)

    def w_copy(h):
        return pltpu.make_async_copy(w_hbm.at[:, pl.ds(pl.multiple_of((2 * sp + h) * cols, cols), cols)], w.at[h], w_sem.at[h])

    def hid_copy(h):
        return pltpu.make_async_copy(hid_hbm.at[:, pl.ds(pl.multiple_of((2 * sp + h) * cols, cols), cols)], hid.at[h], w_sem.at[2 + h])

    w_copy(1 - y).start()
    pl.semaphore_wait(barrier, 3)

    def copy(kind, j, src, dst, dev):
        return pltpu.make_async_remote_copy(src_ref=src, dst_ref=dst, send_sem=send.at[kind, j], recv_sem=recv.at[kind, j], device_id=dev, device_id_type=MESH)

    def at(j):
        return pl.ds(*pieces[j])

    def local(j):
        return pl.ds(pieces[j][0] - first, pieces[j][1])

    pending = []

    def push(cp):
        cp.start()
        pending.append(cp)

    b_range = range(1, count)
    stat_c = copy(0, 0, oth_b.at[half], r1.at[half], to_c)
    push(stat_c)
    o_copies = {j: copy(1, j, oth_b.at[pl.ds(0, half), local(j)], r1.at[pl.ds(0, half), local(j)], to_c) for j in b_range}
    for j in b_range:
        push(o_copies[j])

    own_att = att.at[pl.ds(c * half, half)]
    att_copies = [copy(4, j, own_att.at[:, at(j)], own_att.at[:, at(j)], to_c) for j in range(count)]
    part_copies = [copy(5, u, part.at[1 - y, pl.ds(*unit)], r3.at[1 - y, pl.ds(*unit)], to_y) for u, unit in enumerate(units)]

    parts_a = (own_a, core_a, x_a, diag_a)
    _, total, scales = weigh([p[half] for p in parts_a])
    scales = [s / total for s in scales]
    for h in range(half):
        att[c * half + h, at(0)] = sum(p[h] * s[:, h:h + 1] for p, s in zip(parts_a, scales))
    push(att_copies[0])

    stat_c.wait_recv()
    top, total, scales = weigh([own_b[half], r1[half]])
    c1[half] = jnp.concatenate([top, total, jnp.zeros((own_b.shape[1], head_dim - 2 * half), jnp.float32)], axis=1)
    stat_x = copy(2, 0, c1.at[half], r2.at[half], to_x)
    push(stat_x)
    x_copies = {j: copy(3, j, c1.at[pl.ds(0, half), local(j)], r2.at[pl.ds(0, half), local(j)], to_x) for j in b_range}
    for j in b_range:
        o_copies[j].wait_recv()
        lo, n = pieces[j][0] - first, pieces[j][1]
        for h in range(half):
            c1[h, local(j)] = own_b[h, local(j)] * scales[0][lo:lo + n, h:h + 1] + r1[h, local(j)] * scales[1][lo:lo + n, h:h + 1]
        push(x_copies[j])
    w_copy(y).start()
    for h in range(2):
        hid_copy(h).start()

    def spread(kind, u, blk, dev):
        rows = pl.ds(*units[u])
        return copy(kind, u, yall.at[blk, rows], yall.at[blk, rows], dev)

    b_x, b_y, b_xy = block(1 - x, c, y), block(x, c, 1 - y), block(1 - x, c, 1 - y)
    final = {}

    def finish_heads(j):
        if j == 0:
            return
        if j == 1:
            stat_x.wait_recv()
            _, tot, sc = weigh([c1[half], r2[half]])
            final['scales'] = [s / tot for s in sc]
        x_copies[j].wait_recv()
        lo, n = pieces[j][0] - first, pieces[j][1]
        for h in range(half):
            att[c * half + h, at(j)] = sum(p[h, local(j)] * s[lo:lo + n, h:h + 1] for p, s in zip((c1, r2), final['scales']))
        push(att_copies[j])

    def multiply(j):
        att_copies[j].wait_recv()
        n = pieces[j][1]
        for h in range(heads):
            lhs[:n, h * head_dim:(h + 1) * head_dim] = att[h, at(j)].astype(jnp.bfloat16)

        def tiles(side):
            def tile(i, carry):
                sl = pl.ds(pl.multiple_of(i * 256, 256), 256)
                part[side, at(j), sl] = jnp.dot(lhs[:n], w[side, :, sl], preferred_element_type=jnp.float32)
                return carry
            lax.fori_loop(0, cols // 256, tile, 0)

        if j == 0:
            w_copy(1 - y).wait()
        tiles(1 - y)
        for u in units_of[j]:
            push(part_copies[u])
        if j == 0:
            w_copy(y).wait()
        tiles(y)
        if direct[j]:
            for u in units_of[j]:
                push(both_copy(u))

    def both_copy(u):
        return copy(13, u, part.at[y, pl.ds(*units[u])], r3.at[y, pl.ds(*units[u])], to_y)

    def finish_sum(u):
        if u == 0:
            for h in range(2):
                hid_copy(h).wait()
        rows = pl.ds(*units[u])
        part_copies[u].wait_recv()
        if UNITS[u][2] == 'D':
            both_copy(u).wait_recv()
            for side in range(2):
                yall[block(x, c, side), rows] = hid[side, rows].astype(jnp.float32) + (part[side, rows] + r3[side, rows])
            push(spread(7, u, mine, to_x))
            push(spread(10, u, b_y, to_x))
            push(spread(6, u, mine, to_c))
            push(spread(11, u, b_y, to_c))
            return
        yall[mine, rows] = hid[y, rows].astype(jnp.float32) + (part[y, rows] + r3[y, rows])
        push(spread(8, u, mine, to_y))
        push(spread(7, u, mine, to_x))
        push(spread(6, u, mine, to_c))

    def forward(u):
        mode = UNITS[u][2]

        def from_x():
            spread(7, u, b_x, to_x).wait_recv()
            if mode == 'P':
                push(spread(10, u, b_x, to_y))
            push(spread(9, u, b_x, to_c))

        def from_y():
            spread(8, u, b_y, to_y).wait_recv()
            if mode == 'Q':
                push(spread(10, u, b_y, to_x))
            push(spread(11, u, b_y, to_c))

        for take in {'P': (from_x, from_y), 'Q': (from_y, from_x), 'D': (from_x,)}[mode]:
            take()

    def forward_last(u):
        spread(10, u, b_xy, to_y).wait_recv()
        push(spread(12, u, b_xy, to_c))

    def emit(u):
        spread(6, u, block(x, 1 - c, y), to_c).wait_recv()
        spread(9, u, block(1 - x, 1 - c, y), to_c).wait_recv()
        spread(11, u, block(x, 1 - c, 1 - y), to_c).wait_recv()
        spread(12, u, block(1 - x, 1 - c, 1 - y), to_c).wait_recv()
        for g in range(8):
            y_ref[pl.ds(*units[u]), g * cols:(g + 1) * cols] = yall[g, pl.ds(*units[u])].astype(y_ref.dtype)

    stages = {'h': finish_heads, 's': finish_sum, 'm': multiply, 'f': forward, 'l': forward_last, 'e': emit}
    for name in ORDER.split():
        stages[name[0]](int(name[1:]))
    for cp in pending:
        cp.wait_send()


def combine_and_project(parts_a, parts_b, w_o, hidden):
    ext, nb_a, head_dim = parts_a[0].shape
    nb_b = parts_b[0].shape[1]
    batch = nb_a + nb_b
    half = ext - 1
    heads = 2 * half
    cols = w_o.shape[1] // 8
    f32 = jnp.float32
    kinds, count = 14, max(len(PIECES), len(UNITS))
    return pl.pallas_call(
        combine_kernel,
        out_shape=jax.ShapeDtypeStruct(hidden.shape, hidden.dtype),
        in_specs=[VMEM] * 6 + [ANY, ANY],
        out_specs=VMEM,
        scratch_shapes=[
            pltpu.VMEM((2, w_o.shape[0], cols), w_o.dtype),
            pltpu.VMEM((2, batch, cols), hidden.dtype),
            pltpu.VMEM((ext, nb_b, head_dim), f32),
            pltpu.VMEM((ext, nb_b, head_dim), f32),
            pltpu.VMEM((ext, nb_b, head_dim), f32),
            pltpu.VMEM((heads, batch, head_dim), f32),
            pltpu.VMEM((max(PIECES), heads * head_dim), jnp.bfloat16),
            pltpu.VMEM((2, batch, cols), f32),
            pltpu.VMEM((2, batch, cols), f32),
            pltpu.VMEM((8, batch, cols), f32),
            pltpu.SemaphoreType.DMA((4,)),
            pltpu.SemaphoreType.DMA((kinds, count)),
            pltpu.SemaphoreType.DMA((kinds, count)),
        ],
        compiler_params=pltpu.CompilerParams(collective_id=1, has_side_effects=True, vmem_limit_bytes=38 * 1024 * 1024),
        name='combine',
    )(*parts_a, *parts_b, w_o, hidden)


K_PIECES = 8
N_TILE = 1024
AHEAD = 8


def project_kernel(hid_hbm, gain_hbm, len_hbm, freq_hbm, wq_hbm, wk_hbm, wv_hbm, q_ref, kv_ref, hid_ref, gain_ref, len_ref, freq_ref, cos_ref, sin_ref, gain32, normed, acc, kv_acc, wbuf, kv_buf, hid_sem, w_sem, send, recv):
    batch, depth = hid_ref.shape
    head_dim = cos_ref.shape[1]
    q_cols = wq_hbm.shape[1] // 2
    kv_cols = wk_hbm.shape[1]
    k_rows = depth // K_PIECES
    q_tiles = q_cols // N_TILE
    sp = lax.axis_index('sp')
    c = lax.rem(sp, 2)
    to_c = {'sp': sp + 1 - 2 * c}

    barrier = pltpu.get_barrier_semaphore()
    pl.semaphore_signal(barrier, inc=1, device_id=to_c, device_id_type=MESH)

    def fetch(n, k):
        rows = pl.ds(k * k_rows, k_rows)
        if n == q_tiles:
            return tuple(pltpu.make_async_copy(src.at[rows], kv_buf.at[k], w_sem.at[n, k]) for src in (wk_hbm, wv_hbm))
        col = pl.ds(pl.multiple_of(c * q_cols + n * N_TILE, N_TILE), N_TILE)
        return (pltpu.make_async_copy(wq_hbm.at[rows, col], wbuf.at[n, k], w_sem.at[n, k]),)

    def start(n, k):
        cps = fetch(n, k)
        if n < q_tiles:
            cps[0].start()
            return
        for core in range(2):
            @pl.when(c == core)
            def _(core=core):
                cps[core].start()

    small = [pltpu.make_async_copy(src, dst, hid_sem.at[i]) for i, (src, dst) in enumerate(
        ((hid_hbm, hid_ref), (gain_hbm, gain_ref), (len_hbm, len_ref), (freq_hbm, freq_ref)))]
    for cp in small:
        cp.start()
    order = [piece for k in range(K_PIECES) for piece in ((0, k), (q_tiles, k))]
    order += [(n, k) for n in range(1, q_tiles) for k in range(K_PIECES)]
    for piece in order[:AHEAD]:
        start(*piece)

    def angle_tables():
        angles = jnp.broadcast_to(len_ref[...].astype(jnp.float32), (batch, batch)).T[:, :head_dim] * jnp.concatenate([freq_ref[...]] * 2, axis=1)
        sin_ang = jnp.sin(angles)
        cos_ref[...] = jnp.cos(angles)
        sin_ref[...] = jnp.where(lax.broadcasted_iota(jnp.int32, angles.shape, 1) < head_dim // 2, -sin_ang, sin_ang)

    for cp in small:
        cp.wait()
    gain32[...] = gain_ref[...].astype(jnp.float32)
    step = 1024
    total = jnp.zeros((batch, 1), jnp.float32)
    for j in range(depth // step):
        part = hid_ref[:, j * step:(j + 1) * step].astype(jnp.float32)
        total = total + jnp.sum(part * part, axis=-1, keepdims=True)
    inv_rms = lax.rsqrt(total / depth + NORM_EPS)
    lanes = gain_ref.shape[1]

    def normalize(k):
        for j in range(k * k_rows // lanes, (k + 1) * k_rows // lanes):
            sl = slice(j * lanes, (j + 1) * lanes)
            normed[:, sl] = (hid_ref[:, sl].astype(jnp.float32) * inv_rms * gain32[j:j + 1, :]).astype(normed.dtype)

    def round_bf16(v):
        return v.astype(jnp.bfloat16).astype(jnp.float32)

    def rope(v):
        return round_bf16(v * cos_ref[...] + pltpu.roll(v, head_dim // 2, 1) * sin_ref[...])

    sends = []

    def push(slot, ref, index):
        cp = pltpu.make_async_remote_copy(src_ref=ref.at[index], dst_ref=ref.at[index], send_sem=send.at[slot], recv_sem=recv.at[slot], device_id=to_c, device_id_type=MESH)
        if not sends:
            pl.semaphore_wait(barrier, 1)
        cp.start()
        sends.append(cp)

    per = N_TILE // head_dim

    def epilogue_kv():
        for h in range(kv_cols // head_dim):
            v = round_bf16(kv_acc[:, h * head_dim:(h + 1) * head_dim])
            kv_ref[c, :, h, :] = jnp.where(c == 0, rope(v), v)
        push(q_tiles, kv_ref, c)

    def epilogue(n):
        for h in range(per):
            q_ref[c, :, n * per + h, :] = rope(round_bf16(acc[n % 2, :, h * head_dim:(h + 1) * head_dim]))
        push(n, q_ref, (c, slice(None), pl.ds(n * per, per)))

    for i, (n, k) in enumerate(order):
        fetch(n, k)[0].wait()
        if i + AHEAD < len(order):
            start(*order[i + AHEAD])
        if n == 0:
            normalize(k)
        lhs = normed[:, k * k_rows:(k + 1) * k_rows]
        if n == q_tiles:
            prod = jnp.dot(lhs, kv_buf[k], preferred_element_type=jnp.float32)
            kv_acc[...] = prod + kv_acc[...] if k else prod
        else:
            prod = jnp.dot(lhs, wbuf[n, k], preferred_element_type=jnp.float32)
            acc[n % 2] = prod + acc[n % 2] if k else prod
        if (n, k) == (0, 3):
            angle_tables()
        if (n, k) == (1, 1):
            epilogue_kv()
        if 0 < n < q_tiles and k == 2:
            epilogue(n - 1)
    epilogue(q_tiles - 1)
    for cp in sends:
        cp.wait()


def project(hidden, lengths, norm_gain, w_q, w_k, w_v, inv_freq):
    batch, depth = hidden.shape
    head_dim = 2 * inv_freq.shape[0]
    q_heads = w_q.shape[1] // 2 // head_dim
    kv_heads = w_k.shape[1] // head_dim
    q_tiles = w_q.shape[1] // 2 // N_TILE
    return pl.pallas_call(
        project_kernel,
        out_shape=(jax.ShapeDtypeStruct((2, batch, q_heads, head_dim), jnp.float32), jax.ShapeDtypeStruct((2, batch, kv_heads, head_dim), jnp.float32)),
        in_specs=[HBM] * 7,
        out_specs=(VMEM, VMEM),
        scratch_shapes=[
            pltpu.VMEM((batch, depth), hidden.dtype),
            pltpu.VMEM((depth // 128, 128), norm_gain.dtype),
            pltpu.VMEM((1, batch), jnp.int32),
            pltpu.VMEM((1, head_dim // 2), jnp.float32),
            pltpu.VMEM((batch, head_dim), jnp.float32),
            pltpu.VMEM((batch, head_dim), jnp.float32),
            pltpu.VMEM((depth // 128, 128), jnp.float32),
            pltpu.VMEM((batch, depth), jnp.bfloat16),
            pltpu.VMEM((2, batch, N_TILE), jnp.float32),
            pltpu.VMEM((batch, w_k.shape[1]), jnp.float32),
            pltpu.VMEM((q_tiles, K_PIECES, depth // K_PIECES, N_TILE), w_q.dtype),
            pltpu.VMEM((K_PIECES, depth // K_PIECES, w_k.shape[1]), w_k.dtype),
            pltpu.SemaphoreType.DMA((4,)),
            pltpu.SemaphoreType.DMA((q_tiles + 1, K_PIECES)),
            pltpu.SemaphoreType.DMA((q_tiles + 1,)),
            pltpu.SemaphoreType.DMA((q_tiles + 1,)),
        ],
        compiler_params=pltpu.CompilerParams(collective_id=0, has_side_effects=True, vmem_limit_bytes=50 * 1024 * 1024),
        name='project',
    )(hidden, norm_gain.reshape(depth // 128, 128), lengths.reshape(1, batch), inv_freq.reshape(1, head_dim // 2), w_q, w_k, w_v)


def device_step(hidden, lengths, k_cache, v_cache, norm_gain, w_q, w_k, w_v, w_o, inv_freq):
    batch, slots, kv_local, head_dim = k_cache.shape
    q_all, kv_all = project(hidden, lengths, norm_gain, w_q, w_k, w_v, inv_freq)
    flat = (batch, slots * kv_local, head_dim)
    shared = (lengths, q_all, kv_all, k_cache.reshape(flat), v_cache.reshape(flat))
    k_upd, v_upd, own_a, oth_a = write_and_attend(0, FIRST, *shared)
    swap = lambda array, flip: lax.ppermute(array, 'sp', [(s, s ^ flip) for s in range(4)])
    parts_a = (own_a, swap(oth_a, 1), swap(own_a, 2), swap(oth_a, 3))
    k_upd, v_upd, own_b, oth_b = write_and_attend(FIRST, batch - FIRST, *shared, written=(k_upd, v_upd))
    y_out = combine_and_project(parts_a, (own_b, oth_b), w_o, hidden)
    return y_out, k_upd.reshape(k_cache.shape), v_upd.reshape(v_cache.shape)


def solution(mesh):
    cache_spec = P('dp', 'sp', 'tp', None)
    in_specs = (P('dp', None), P('dp'), cache_spec, cache_spec, P(None), P(None, 'tp'), P(None, 'tp'), P(None, 'tp'), P('tp', None), P(None))
    out_specs = (P('dp', None), cache_spec, cache_spec)
    return jax.shard_map(device_step, mesh=mesh, in_specs=in_specs, out_specs=out_specs, check_vma=False)
```

```python
import functools

import jax
import jax.numpy as jnp
from jax import lax
from jax.experimental import pallas as pl
from jax.experimental.pallas import tpu as pltpu
from jax.sharding import PartitionSpec as P

NORM_EPS = 1e-5
NEG_BIG = -3.0e38
LOG2E = 1.4426950408889634
ANY = pl.BlockSpec(memory_space=pl.ANY)
HBM = pl.BlockSpec(memory_space=pltpu.HBM)
VMEM = pl.BlockSpec(memory_space=pltpu.VMEM)
SMEM = pl.BlockSpec(memory_space=pltpu.SMEM)


CHUNK = 8
PART = 4
NBUF = 5
LAG = 2


def attend_kernel(first, count, len_ref, q_hbm, kv_hbm, k_hbm, v_hbm, *refs):
    ko_hbm, vo_hbm, own_ref, oth_ref, q_ref, kv_ref, kbuf, vbuf, obuf, mbuf, lbuf, in_sem, out_sem, q_sem = refs[-14:]
    batch, rows, head_dim = k_hbm.shape
    kv_local = kv_ref.shape[2]
    heads = 2 * q_ref.shape[2]
    slots = rows // kv_local
    steps = count // CHUNK
    slot_start = lax.axis_index('sp') * slots

    def copies_in(i, part):
        b = lax.rem(i, NBUF)
        src = pl.ds(first + i * CHUNK + part * PART, PART)
        dst = pl.ds(part * PART, PART)
        return (pltpu.make_async_copy(k_hbm.at[src], kbuf.at[b, dst], in_sem.at[0, b, part]),
                pltpu.make_async_copy(v_hbm.at[src], vbuf.at[b, dst], in_sem.at[1, b, part]))

    def copies_out(i, part):
        b = lax.rem(i, NBUF)
        src = pl.ds(part * PART, PART)
        dst = pl.ds(first + i * CHUNK + part * PART, PART)
        return (pltpu.make_async_copy(kbuf.at[b, src], ko_hbm.at[dst], out_sem.at[0, b, part]),
                pltpu.make_async_copy(vbuf.at[b, src], vo_hbm.at[dst], out_sem.at[1, b, part]))

    parts = range(CHUNK // PART)
    small = (pltpu.make_async_copy(q_hbm.at[:, pl.ds(first, count)], q_ref, q_sem.at[0]), pltpu.make_async_copy(kv_hbm.at[:, pl.ds(first, count)], kv_ref, q_sem.at[1]))
    for cp in small:
        cp.start()
    for i in range(NBUF - LAG):
        for part in parts:
            for cp in copies_in(i, part):
                cp.start()

    col = lax.broadcasted_iota(jnp.int32, (heads, rows), 1)
    row = lax.broadcasted_iota(jnp.int32, (heads, rows), 0)
    head_ok = lax.rem(col, kv_local) == row // (heads // kv_local)
    tile_slot = lax.broadcasted_iota(jnp.int32, (16, head_dim), 0) // kv_local
    lane = lax.broadcasted_iota(jnp.int32, (heads, batch), 1)
    score_scale = head_dim ** -0.5 * LOG2E
    half = heads // 2
    core = lax.rem(lax.axis_index('sp'), 2)

    def store_token(i, s):
        buf = lax.rem(i, NBUF)
        b = first + i * CHUNK + s
        pos = len_ref[b] - slot_start
        own = (pos >= 0) & (pos < slots)
        safe = jnp.where(own, pos, 0)
        per_tile = 16 // kv_local
        base = pl.multiple_of(safe // per_tile * 16, 16)
        pick = (tile_slot == lax.rem(safe, per_tile)) & own
        for dst, which in ((kbuf, 0), (vbuf, 1)):
            new = jnp.concatenate([kv_ref[which, b - first]] * per_tile, axis=0)
            old = dst[buf, s, pl.ds(base, 16), :].astype(jnp.float32)
            dst[buf, s, pl.ds(base, 16), :] = jnp.where(pick, new, old).astype(jnp.bfloat16)

    def attend_pair(i, s, m_all, l_all):
        buf = lax.rem(i, NBUF)
        b0 = first + i * CHUNK + s
        b1 = b0 + 1
        limit0 = (len_ref[b0] - slot_start + 1) * kv_local
        limit1 = (len_ref[b1] - slot_start + 1) * kv_local
        q0 = jnp.concatenate([q_ref[0, b0 - first], q_ref[1, b0 - first]], axis=0).astype(jnp.bfloat16)
        q1 = jnp.concatenate([q_ref[0, b1 - first], q_ref[1, b1 - first]], axis=0).astype(jnp.bfloat16)
        zero = jnp.zeros_like(q0)
        q = jnp.concatenate([jnp.concatenate([q0, zero], axis=1), jnp.concatenate([zero, q1], axis=1)], axis=0)
        k = jnp.concatenate([kbuf[buf, s], kbuf[buf, s + 1]], axis=1)
        v = jnp.concatenate([vbuf[buf, s], vbuf[buf, s + 1]], axis=1)
        scores = lax.dot_general(q, k, (((1,), (1,)), ((), ())), preferred_element_type=jnp.float32)
        valid = jnp.concatenate([head_ok & (col < limit0), head_ok & (col < limit1)], axis=0)
        scores = jnp.where(valid, scores * score_scale, NEG_BIG)
        top = jnp.max(scores, axis=-1, keepdims=True)
        weights = jnp.where(valid, jnp.exp2(scores - top), 0.0)
        total = jnp.sum(weights, axis=-1, keepdims=True)
        out = jnp.dot(weights.astype(jnp.bfloat16), v, preferred_element_type=jnp.float32)
        obuf[s] = out[:heads, :head_dim]
        obuf[s + 1] = out[heads:, head_dim:]
        m_all = jnp.where(lane == b0, top[:heads], jnp.where(lane == b1, top[heads:], m_all))
        l_all = jnp.where(lane == b0, total[:heads], jnp.where(lane == b1, total[heads:], l_all))
        return m_all, l_all

    def step(i, carry):
        for part in parts:
            @pl.when((i >= LAG) & (i + NBUF - LAG < steps))
            def _():
                for cp in copies_out(i - LAG, part):
                    cp.wait()

            @pl.when(i + NBUF - LAG < steps)
            def _():
                for cp in copies_in(i + NBUF - LAG, part):
                    cp.start()

        m_all, l_all = mbuf[...], lbuf[...]
        for part in parts:
            for cp in copies_in(i, part):
                cp.wait()
            for s in range(part * PART, (part + 1) * PART):
                store_token(i, s)
            for s in range(part * PART, (part + 1) * PART, 2):
                m_all, l_all = attend_pair(i, s, m_all, l_all)
            for cp in copies_out(i, part):
                cp.start()
        mbuf[...] = m_all
        lbuf[...] = l_all
        out_rows = pl.ds(pl.multiple_of(i * CHUNK, CHUNK), CHUNK)
        by_head = jnp.swapaxes(obuf[...], 0, 1)
        own_ref[:half, out_rows] = jnp.where(core == 0, by_head[:half], by_head[half:])
        oth_ref[:half, out_rows] = jnp.where(core == 0, by_head[half:], by_head[:half])

        return carry

    mbuf[...] = jnp.zeros_like(mbuf)
    lbuf[...] = jnp.zeros_like(lbuf)
    for cp in small:
        cp.wait()
    lax.fori_loop(0, steps, step, 0)
    for i in range(steps - NBUF, steps):
        for part in parts:
            for cp in copies_out(i, part):
                cp.wait()
    stats = []
    for lo in (0, half):
        rows_ml = [mbuf[lo:lo + half], lbuf[lo:lo + half], jnp.zeros((batch - 2 * half, batch), jnp.float32)]
        stats.append(jnp.concatenate(rows_ml, axis=0).T[first:first + count])
    own_ref[half] = jnp.where(core == 0, stats[0], stats[1])
    oth_ref[half] = jnp.where(core == 0, stats[1], stats[0])


def write_and_attend(first, count, lengths, q_all, kv_all, k_cache, v_cache, written=()):
    batch, rows, head_dim = k_cache.shape
    heads = q_all.shape[0] * q_all.shape[2]
    part = jax.ShapeDtypeStruct((heads // 2 + 1, count, head_dim), jnp.float32)
    cache = jax.ShapeDtypeStruct(k_cache.shape, k_cache.dtype)
    return pl.pallas_call(
        functools.partial(attend_kernel, first, count),
        out_shape=(cache, cache, part, part),
        in_specs=[SMEM] + [HBM] * 4 + [ANY] * len(written),
        out_specs=(ANY, ANY, VMEM, VMEM),
        input_output_aliases={5: 0, 6: 1} if written else {},
        scratch_shapes=[
            pltpu.VMEM((2, count) + q_all.shape[2:], jnp.float32),
            pltpu.VMEM((2, count) + kv_all.shape[2:], jnp.float32),
            pltpu.VMEM((NBUF, CHUNK, rows, head_dim), jnp.bfloat16),
            pltpu.VMEM((NBUF, CHUNK, rows, head_dim), jnp.bfloat16),
            pltpu.VMEM((CHUNK, heads, head_dim), jnp.float32),
            pltpu.VMEM((heads, batch), jnp.float32),
            pltpu.VMEM((heads, batch), jnp.float32),
            pltpu.SemaphoreType.DMA((2, NBUF, CHUNK // PART)),
            pltpu.SemaphoreType.DMA((2, NBUF, CHUNK // PART)),
            pltpu.SemaphoreType.DMA((2,)),
        ],
        compiler_params=pltpu.CompilerParams(vmem_limit_bytes=34 * 1024 * 1024),
        cost_estimate=pl.CostEstimate(flops=100 * count * heads * rows * head_dim, bytes_accessed=8 * count * rows * head_dim, transcendentals=0),
        name='attend',
    )(lengths, q_all, kv_all, k_cache, v_cache, *written)


FIRST = 64
PIECES = (64, 48, 16)
UNITS = ((0, 32, 'Q'), (0, 32, 'Q'), (1, 24, 'P'), (1, 24, 'P'), (2, 16, 'D'))
ORDER = ('m0', 's0', 's1', 'h1', 'm1', 'h2', 'f0', 'f1', 's2', 'm2', 's3', 'f2', 's4',
         'f3', 'f4', 'l0', 'l1', 'l2', 'l3', 'l4', 'e0', 'e1', 'e2', 'e3', 'e4')
MESH = pl.DeviceIdType.MESH


def weigh(tiles):
    half = 16
    tops = [t[:, :half] for t in tiles]
    top = functools.reduce(jnp.maximum, tops)
    scales = [jnp.exp2(m - top) for m in tops]
    total = sum(t[:, half:2 * half] * s for t, s in zip(tiles, scales))
    return top, total, scales


def combine_kernel(own_a, core_a, x_a, diag_a, own_b, oth_b, w_hbm, hid_hbm, y_ref, w, hid, r1, c1, r2, att, lhs, part, r3, yall,
                   w_sem, send, recv):
    heads, batch, head_dim = att.shape
    half = heads // 2
    cols = part.shape[2]
    first = own_a.shape[1]
    pieces = [(sum(PIECES[:j]), n) for j, n in enumerate(PIECES)]
    count = len(pieces)
    units = [(sum(n for _, n, _ in UNITS[:u]), n) for u, (_, n, _) in enumerate(UNITS)]
    units_of = [[u for u, unit in enumerate(UNITS) if unit[0] == j] for j in range(count)]
    direct = [UNITS[us[0]][2] == 'D' for us in units_of]
    sp, y = lax.axis_index('sp'), lax.axis_index('tp')
    c, x = lax.rem(sp, 2), sp // 2
    to_c, to_x, to_y = {'sp': sp + 1 - 2 * c}, {'sp': sp + 2 - 4 * x}, {'tp': 1 - y}
    block = lambda xx, cc, yy: 4 * xx + 2 * cc + yy
    mine = block(x, c, y)

    barrier = pltpu.get_barrier_semaphore()
    for dev in (to_c, to_x, to_y):
        pl.semaphore_signal(barrier, inc=1, device_id=dev, device_id_type=MESH)

    def w_copy(h):
        return pltpu.make_async_copy(w_hbm.at[:, pl.ds(pl.multiple_of((2 * sp + h) * cols, cols), cols)], w.at[h], w_sem.at[h])

    def hid_copy(h):
        return pltpu.make_async_copy(hid_hbm.at[:, pl.ds(pl.multiple_of((2 * sp + h) * cols, cols), cols)], hid.at[h], w_sem.at[2 + h])

    w_copy(1 - y).start()
    pl.semaphore_wait(barrier, 3)

    def copy(kind, j, src, dst, dev):
        return pltpu.make_async_remote_copy(src_ref=src, dst_ref=dst, send_sem=send.at[kind, j], recv_sem=recv.at[kind, j], device_id=dev, device_id_type=MESH)

    def at(j):
        return pl.ds(*pieces[j])

    def local(j):
        return pl.ds(pieces[j][0] - first, pieces[j][1])

    pending = []

    def push(cp):
        cp.start()
        pending.append(cp)

    b_range = range(1, count)
    stat_c = copy(0, 0, oth_b.at[half], r1.at[half], to_c)
    push(stat_c)
    o_copies = {j: copy(1, j, oth_b.at[pl.ds(0, half), local(j)], r1.at[pl.ds(0, half), local(j)], to_c) for j in b_range}
    for j in b_range:
        push(o_copies[j])

    own_att = att.at[pl.ds(c * half, half)]
    att_copies = [copy(4, j, own_att.at[:, at(j)], own_att.at[:, at(j)], to_c) for j in range(count)]
    part_copies = [copy(5, u, part.at[1 - y, pl.ds(*unit)], r3.at[1 - y, pl.ds(*unit)], to_y) for u, unit in enumerate(units)]

    parts_a = (own_a, core_a, x_a, diag_a)
    _, total, scales = weigh([p[half] for p in parts_a])
    scales = [s / total for s in scales]
    for h in range(half):
        att[c * half + h, at(0)] = sum(p[h] * s[:, h:h + 1] for p, s in zip(parts_a, scales))
    push(att_copies[0])

    stat_c.wait_recv()
    top, total, scales = weigh([own_b[half], r1[half]])
    c1[half] = jnp.concatenate([top, total, jnp.zeros((own_b.shape[1], head_dim - 2 * half), jnp.float32)], axis=1)
    stat_x = copy(2, 0, c1.at[half], r2.at[half], to_x)
    push(stat_x)
    x_copies = {j: copy(3, j, c1.at[pl.ds(0, half), local(j)], r2.at[pl.ds(0, half), local(j)], to_x) for j in b_range}
    for j in b_range:
        o_copies[j].wait_recv()
        lo, n = pieces[j][0] - first, pieces[j][1]
        for h in range(half):
            c1[h, local(j)] = own_b[h, local(j)] * scales[0][lo:lo + n, h:h + 1] + r1[h, local(j)] * scales[1][lo:lo + n, h:h + 1]
        push(x_copies[j])
    w_copy(y).start()
    for h in range(2):
        hid_copy(h).start()

    def spread(kind, u, blk, dev):
        rows = pl.ds(*units[u])
        return copy(kind, u, yall.at[blk, rows], yall.at[blk, rows], dev)

    b_x, b_y, b_xy = block(1 - x, c, y), block(x, c, 1 - y), block(1 - x, c, 1 - y)
    final = {}

    def finish_heads(j):
        if j == 0:
            return
        if j == 1:
            stat_x.wait_recv()
            _, tot, sc = weigh([c1[half], r2[half]])
            final['scales'] = [s / tot for s in sc]
        x_copies[j].wait_recv()
        lo, n = pieces[j][0] - first, pieces[j][1]
        for h in range(half):
            att[c * half + h, at(j)] = sum(p[h, local(j)] * s[lo:lo + n, h:h + 1] for p, s in zip((c1, r2), final['scales']))
        push(att_copies[j])

    def multiply(j):
        att_copies[j].wait_recv()
        n = pieces[j][1]
        for h in range(heads):
            lhs[:n, h * head_dim:(h + 1) * head_dim] = att[h, at(j)].astype(jnp.bfloat16)

        def tiles(side):
            def tile(i, carry):
                sl = pl.ds(pl.multiple_of(i * 256, 256), 256)
                part[side, at(j), sl] = jnp.dot(lhs[:n], w[side, :, sl], preferred_element_type=jnp.float32)
                return carry
            lax.fori_loop(0, cols // 256, tile, 0)

        if j == 0:
            w_copy(1 - y).wait()
        tiles(1 - y)
        for u in units_of[j]:
            push(part_copies[u])
        if j == 0:
            w_copy(y).wait()
        tiles(y)
        if direct[j]:
            for u in units_of[j]:
                push(both_copy(u))

    def both_copy(u):
        return copy(13, u, part.at[y, pl.ds(*units[u])], r3.at[y, pl.ds(*units[u])], to_y)

    def finish_sum(u):
        if u == 0:
            for h in range(2):
                hid_copy(h).wait()
        rows = pl.ds(*units[u])
        part_copies[u].wait_recv()
        if UNITS[u][2] == 'D':
            both_copy(u).wait_recv()
            for side in range(2):
                yall[block(x, c, side), rows] = hid[side, rows].astype(jnp.float32) + (part[side, rows] + r3[side, rows])
            push(spread(7, u, mine, to_x))
            push(spread(10, u, b_y, to_x))
            push(spread(6, u, mine, to_c))
            push(spread(11, u, b_y, to_c))
            return
        yall[mine, rows] = hid[y, rows].astype(jnp.float32) + (part[y, rows] + r3[y, rows])
        push(spread(8, u, mine, to_y))
        push(spread(7, u, mine, to_x))
        push(spread(6, u, mine, to_c))

    def forward(u):
        mode = UNITS[u][2]

        def from_x():
            spread(7, u, b_x, to_x).wait_recv()
            if mode == 'P':
                push(spread(10, u, b_x, to_y))
            push(spread(9, u, b_x, to_c))

        def from_y():
            spread(8, u, b_y, to_y).wait_recv()
            if mode == 'Q':
                push(spread(10, u, b_y, to_x))
            push(spread(11, u, b_y, to_c))

        for take in {'P': (from_x, from_y), 'Q': (from_y, from_x), 'D': (from_x,)}[mode]:
            take()

    def forward_last(u):
        spread(10, u, b_xy, to_y).wait_recv()
        push(spread(12, u, b_xy, to_c))

    def emit(u):
        spread(6, u, block(x, 1 - c, y), to_c).wait_recv()
        spread(9, u, block(1 - x, 1 - c, y), to_c).wait_recv()
        spread(11, u, block(x, 1 - c, 1 - y), to_c).wait_recv()
        spread(12, u, block(1 - x, 1 - c, 1 - y), to_c).wait_recv()
        for g in range(8):
            y_ref[pl.ds(*units[u]), g * cols:(g + 1) * cols] = yall[g, pl.ds(*units[u])].astype(y_ref.dtype)

    stages = {'h': finish_heads, 's': finish_sum, 'm': multiply, 'f': forward, 'l': forward_last, 'e': emit}
    for name in ORDER:
        stages[name[0]](int(name[1:]))
    for cp in pending:
        cp.wait_send()


def combine_and_project(parts_a, parts_b, w_o, hidden):
    ext, nb_a, head_dim = parts_a[0].shape
    nb_b = parts_b[0].shape[1]
    batch = nb_a + nb_b
    half = ext - 1
    heads = 2 * half
    cols = w_o.shape[1] // 8
    f32 = jnp.float32
    kinds, count = 14, max(len(PIECES), len(UNITS))
    return pl.pallas_call(
        combine_kernel,
        out_shape=jax.ShapeDtypeStruct(hidden.shape, hidden.dtype),
        in_specs=[VMEM] * 6 + [ANY, ANY],
        out_specs=VMEM,
        scratch_shapes=[
            pltpu.VMEM((2, w_o.shape[0], cols), w_o.dtype),
            pltpu.VMEM((2, batch, cols), hidden.dtype),
            pltpu.VMEM((ext, nb_b, head_dim), f32),
            pltpu.VMEM((ext, nb_b, head_dim), f32),
            pltpu.VMEM((ext, nb_b, head_dim), f32),
            pltpu.VMEM((heads, batch, head_dim), f32),
            pltpu.VMEM((max(PIECES), heads * head_dim), jnp.bfloat16),
            pltpu.VMEM((2, batch, cols), f32),
            pltpu.VMEM((2, batch, cols), f32),
            pltpu.VMEM((8, batch, cols), f32),
            pltpu.SemaphoreType.DMA((4,)),
            pltpu.SemaphoreType.DMA((kinds, count)),
            pltpu.SemaphoreType.DMA((kinds, count)),
        ],
        compiler_params=pltpu.CompilerParams(collective_id=1, has_side_effects=True, vmem_limit_bytes=38 * 1024 * 1024),
        name='combine',
    )(*parts_a, *parts_b, w_o, hidden)


K_PIECES = 8
N_TILE = 1024
AHEAD = 8


def project_kernel(hid_hbm, gain_hbm, len_hbm, freq_hbm, wq_hbm, wk_hbm, wv_hbm, q_ref, kv_ref, hid_ref, gain_ref, len_ref, freq_ref, cos_ref, sin_ref, gain32, normed, acc, kv_acc, wbuf, kv_buf, hid_sem, w_sem, send, recv):
    batch, depth = hid_ref.shape
    head_dim = cos_ref.shape[1]
    q_cols = wq_hbm.shape[1] // 2
    kv_cols = wk_hbm.shape[1]
    k_rows = depth // K_PIECES
    q_tiles = q_cols // N_TILE
    sp = lax.axis_index('sp')
    c = lax.rem(sp, 2)
    to_c = {'sp': sp + 1 - 2 * c}

    barrier = pltpu.get_barrier_semaphore()
    pl.semaphore_signal(barrier, inc=1, device_id=to_c, device_id_type=MESH)

    def fetch(n, k):
        rows = pl.ds(k * k_rows, k_rows)
        if n == q_tiles:
            return tuple(pltpu.make_async_copy(src.at[rows], kv_buf.at[k], w_sem.at[n, k]) for src in (wk_hbm, wv_hbm))
        col = pl.ds(pl.multiple_of(c * q_cols + n * N_TILE, N_TILE), N_TILE)
        return (pltpu.make_async_copy(wq_hbm.at[rows, col], wbuf.at[n, k], w_sem.at[n, k]),)

    def start(n, k):
        cps = fetch(n, k)
        if n < q_tiles:
            cps[0].start()
            return
        for core in range(2):
            @pl.when(c == core)
            def _(core=core):
                cps[core].start()

    small = [pltpu.make_async_copy(src, dst, hid_sem.at[i]) for i, (src, dst) in enumerate(
        ((hid_hbm, hid_ref), (gain_hbm, gain_ref), (len_hbm, len_ref), (freq_hbm, freq_ref)))]
    for cp in small:
        cp.start()
    order = [piece for k in range(K_PIECES) for piece in ((0, k), (q_tiles, k))]
    order += [(n, k) for n in range(1, q_tiles) for k in range(K_PIECES)]
    for piece in order[:AHEAD]:
        start(*piece)

    def angle_tables():
        angles = jnp.broadcast_to(len_ref[...].astype(jnp.float32), (batch, batch)).T[:, :head_dim] * jnp.concatenate([freq_ref[...]] * 2, axis=1)
        sin_ang = jnp.sin(angles)
        cos_ref[...] = jnp.cos(angles)
        sin_ref[...] = jnp.where(lax.broadcasted_iota(jnp.int32, angles.shape, 1) < head_dim // 2, -sin_ang, sin_ang)

    for cp in small:
        cp.wait()
    gain32[...] = gain_ref[...].astype(jnp.float32)
    step = 1024
    total = jnp.zeros((batch, 1), jnp.float32)
    for j in range(depth // step):
        part = hid_ref[:, j * step:(j + 1) * step].astype(jnp.float32)
        total = total + jnp.sum(part * part, axis=-1, keepdims=True)
    inv_rms = lax.rsqrt(total / depth + NORM_EPS)
    lanes = gain_ref.shape[1]

    def normalize(k):
        for j in range(k * k_rows // lanes, (k + 1) * k_rows // lanes):
            sl = slice(j * lanes, (j + 1) * lanes)
            normed[:, sl] = (hid_ref[:, sl].astype(jnp.float32) * inv_rms * gain32[j:j + 1, :]).astype(normed.dtype)

    def round_bf16(v):
        return v.astype(jnp.bfloat16).astype(jnp.float32)

    def rope(v):
        return round_bf16(v * cos_ref[...] + pltpu.roll(v, head_dim // 2, 1) * sin_ref[...])

    sends = []

    def push(slot, ref, index):
        cp = pltpu.make_async_remote_copy(src_ref=ref.at[index], dst_ref=ref.at[index], send_sem=send.at[slot], recv_sem=recv.at[slot], device_id=to_c, device_id_type=MESH)
        if not sends:
            pl.semaphore_wait(barrier, 1)
        cp.start()
        sends.append(cp)

    per = N_TILE // head_dim

    def epilogue_kv():
        for h in range(kv_cols // head_dim):
            v = round_bf16(kv_acc[:, h * head_dim:(h + 1) * head_dim])
            kv_ref[c, :, h, :] = jnp.where(c == 0, rope(v), v)
        push(q_tiles, kv_ref, c)

    def epilogue(n):
        for h in range(per):
            q_ref[c, :, n * per + h, :] = rope(round_bf16(acc[n % 2, :, h * head_dim:(h + 1) * head_dim]))
        push(n, q_ref, (c, slice(None), pl.ds(n * per, per)))

    for i, (n, k) in enumerate(order):
        fetch(n, k)[0].wait()
        if i + AHEAD < len(order):
            start(*order[i + AHEAD])
        if n == 0:
            normalize(k)
        lhs = normed[:, k * k_rows:(k + 1) * k_rows]
        if n == q_tiles:
            prod = jnp.dot(lhs, kv_buf[k], preferred_element_type=jnp.float32)
            kv_acc[...] = prod + kv_acc[...] if k else prod
        else:
            prod = jnp.dot(lhs, wbuf[n, k], preferred_element_type=jnp.float32)
            acc[n % 2] = prod + acc[n % 2] if k else prod
        if (n, k) == (0, 3):
            angle_tables()
        if (n, k) == (1, 1):
            epilogue_kv()
        if 0 < n < q_tiles and k == 2:
            epilogue(n - 1)
    epilogue(q_tiles - 1)
    for cp in sends:
        cp.wait()


def project(hidden, lengths, norm_gain, w_q, w_k, w_v, inv_freq):
    batch, depth = hidden.shape
    head_dim = 2 * inv_freq.shape[0]
    q_heads = w_q.shape[1] // 2 // head_dim
    kv_heads = w_k.shape[1] // head_dim
    q_tiles = w_q.shape[1] // 2 // N_TILE
    return pl.pallas_call(
        project_kernel,
        out_shape=(jax.ShapeDtypeStruct((2, batch, q_heads, head_dim), jnp.float32), jax.ShapeDtypeStruct((2, batch, kv_heads, head_dim), jnp.float32)),
        in_specs=[HBM] * 7,
        out_specs=(VMEM, VMEM),
        scratch_shapes=[
            pltpu.VMEM((batch, depth), hidden.dtype),
            pltpu.VMEM((depth // 128, 128), norm_gain.dtype),
            pltpu.VMEM((1, batch), jnp.int32),
            pltpu.VMEM((1, head_dim // 2), jnp.float32),
            pltpu.VMEM((batch, head_dim), jnp.float32),
            pltpu.VMEM((batch, head_dim), jnp.float32),
            pltpu.VMEM((depth // 128, 128), jnp.float32),
            pltpu.VMEM((batch, depth), jnp.bfloat16),
            pltpu.VMEM((2, batch, N_TILE), jnp.float32),
            pltpu.VMEM((batch, w_k.shape[1]), jnp.float32),
            pltpu.VMEM((q_tiles, K_PIECES, depth // K_PIECES, N_TILE), w_q.dtype),
            pltpu.VMEM((K_PIECES, depth // K_PIECES, w_k.shape[1]), w_k.dtype),
            pltpu.SemaphoreType.DMA((4,)),
            pltpu.SemaphoreType.DMA((q_tiles + 1, K_PIECES)),
            pltpu.SemaphoreType.DMA((q_tiles + 1,)),
            pltpu.SemaphoreType.DMA((q_tiles + 1,)),
        ],
        compiler_params=pltpu.CompilerParams(collective_id=0, has_side_effects=True, vmem_limit_bytes=50 * 1024 * 1024),
        name='project',
    )(hidden, norm_gain.reshape(depth // 128, 128), lengths.reshape(1, batch), inv_freq.reshape(1, head_dim // 2), w_q, w_k, w_v)


def device_step(hidden, lengths, k_cache, v_cache, norm_gain, w_q, w_k, w_v, w_o, inv_freq):
    batch, slots, kv_local, head_dim = k_cache.shape
    q_all, kv_all = project(hidden, lengths, norm_gain, w_q, w_k, w_v, inv_freq)
    flat = (batch, slots * kv_local, head_dim)
    shared = (lengths, q_all, kv_all, k_cache.reshape(flat), v_cache.reshape(flat))
    k_upd, v_upd, own_a, oth_a = write_and_attend(0, FIRST, *shared)
    swap = lambda array, flip: lax.ppermute(array, 'sp', [(s, s ^ flip) for s in range(4)])
    parts_a = (own_a, swap(oth_a, 1), swap(own_a, 2), swap(oth_a, 3))
    k_upd, v_upd, own_b, oth_b = write_and_attend(FIRST, batch - FIRST, *shared, written=(k_upd, v_upd))
    y_out = combine_and_project(parts_a, (own_b, oth_b), w_o, hidden)
    return y_out, k_upd.reshape(k_cache.shape), v_upd.reshape(v_cache.shape)


def solution(mesh):
    cache_spec = P('dp', 'sp', 'tp', None)
    in_specs = (P('dp', None), P('dp'), cache_spec, cache_spec, P(None), P(None, 'tp'), P(None, 'tp'), P(None, 'tp'), P('tp', None), P(None))
    out_specs = (P('dp', None), cache_spec, cache_spec)
    return jax.shard_map(device_step, mesh=mesh, in_specs=in_specs, out_specs=out_specs, check_vma=False)
```

```python
import functools

import jax
import jax.numpy as jnp
from jax import lax
from jax.experimental import pallas as pl
from jax.experimental.pallas import tpu as pltpu
from jax.sharding import PartitionSpec as P

NORM_EPS = 1e-5
NEG_BIG = -3.0e38
LOG2E = 1.4426950408889634
ANY = pl.BlockSpec(memory_space=pl.ANY)
HBM = pl.BlockSpec(memory_space=pltpu.HBM)
VMEM = pl.BlockSpec(memory_space=pltpu.VMEM)
SMEM = pl.BlockSpec(memory_space=pltpu.SMEM)


CHUNK = 8
PART = 4
NBUF = 5
LAG = 2


def attend_kernel(first, count, len_ref, q_hbm, kv_hbm, k_hbm, v_hbm, *refs):
    ko_hbm, vo_hbm, own_ref, oth_ref, q_ref, kv_ref, kbuf, vbuf, obuf, mbuf, lbuf, in_sem, out_sem, q_sem = refs[-14:]
    batch, rows, head_dim = k_hbm.shape
    kv_local = kv_ref.shape[2]
    heads = 2 * q_ref.shape[2]
    slots = rows // kv_local
    steps = count // CHUNK
    slot_start = lax.axis_index('sp') * slots

    def copies_in(i, part):
        b = lax.rem(i, NBUF)
        src = pl.ds(first + i * CHUNK + part * PART, PART)
        dst = pl.ds(part * PART, PART)
        return (pltpu.make_async_copy(k_hbm.at[src], kbuf.at[b, dst], in_sem.at[0, b, part]),
                pltpu.make_async_copy(v_hbm.at[src], vbuf.at[b, dst], in_sem.at[1, b, part]))

    def copies_out(i, part):
        b = lax.rem(i, NBUF)
        src = pl.ds(part * PART, PART)
        dst = pl.ds(first + i * CHUNK + part * PART, PART)
        return (pltpu.make_async_copy(kbuf.at[b, src], ko_hbm.at[dst], out_sem.at[0, b, part]),
                pltpu.make_async_copy(vbuf.at[b, src], vo_hbm.at[dst], out_sem.at[1, b, part]))

    parts = range(CHUNK // PART)
    small = (pltpu.make_async_copy(q_hbm.at[:, pl.ds(first, count)], q_ref, q_sem.at[0]), pltpu.make_async_copy(kv_hbm.at[:, pl.ds(first, count)], kv_ref, q_sem.at[1]))
    for cp in small:
        cp.start()
    for i in range(NBUF - LAG):
        for part in parts:
            for cp in copies_in(i, part):
                cp.start()

    col = lax.broadcasted_iota(jnp.int32, (heads, rows), 1)
    row = lax.broadcasted_iota(jnp.int32, (heads, rows), 0)
    head_ok = lax.rem(col, kv_local) == row // (heads // kv_local)
    tile_slot = lax.broadcasted_iota(jnp.int32, (16, head_dim), 0) // kv_local
    lane = lax.broadcasted_iota(jnp.int32, (heads, batch), 1)
    score_scale = head_dim ** -0.5 * LOG2E
    half = heads // 2
    core = lax.rem(lax.axis_index('sp'), 2)

    def store_token(i, s):
        buf = lax.rem(i, NBUF)
        b = first + i * CHUNK + s
        pos = len_ref[b] - slot_start
        own = (pos >= 0) & (pos < slots)
        safe = jnp.where(own, pos, 0)
        per_tile = 16 // kv_local
        base = pl.multiple_of(safe // per_tile * 16, 16)
        pick = (tile_slot == lax.rem(safe, per_tile)) & own
        for dst, which in ((kbuf, 0), (vbuf, 1)):
            new = jnp.concatenate([kv_ref[which, b - first]] * per_tile, axis=0)
            old = dst[buf, s, pl.ds(base, 16), :].astype(jnp.float32)
            dst[buf, s, pl.ds(base, 16), :] = jnp.where(pick, new, old).astype(jnp.bfloat16)

    def attend_pair(i, s, m_all, l_all):
        buf = lax.rem(i, NBUF)
        b0 = first + i * CHUNK + s
        b1 = b0 + 1
        limit0 = (len_ref[b0] - slot_start + 1) * kv_local
        limit1 = (len_ref[b1] - slot_start + 1) * kv_local
        q0 = jnp.concatenate([q_ref[0, b0 - first], q_ref[1, b0 - first]], axis=0).astype(jnp.bfloat16)
        q1 = jnp.concatenate([q_ref[0, b1 - first], q_ref[1, b1 - first]], axis=0).astype(jnp.bfloat16)
        zero = jnp.zeros_like(q0)
        q = jnp.concatenate([jnp.concatenate([q0, zero], axis=1), jnp.concatenate([zero, q1], axis=1)], axis=0)
        k = jnp.concatenate([kbuf[buf, s], kbuf[buf, s + 1]], axis=1)
        v = jnp.concatenate([vbuf[buf, s], vbuf[buf, s + 1]], axis=1)
        scores = lax.dot_general(q, k, (((1,), (1,)), ((), ())), preferred_element_type=jnp.float32)
        valid = jnp.concatenate([head_ok & (col < limit0), head_ok & (col < limit1)], axis=0)
        scores = jnp.where(valid, scores * score_scale, NEG_BIG)
        top = jnp.max(scores, axis=-1, keepdims=True)
        weights = jnp.where(valid, jnp.exp2(scores - top), 0.0)
        total = jnp.sum(weights, axis=-1, keepdims=True)
        out = jnp.dot(weights.astype(jnp.bfloat16), v, preferred_element_type=jnp.float32)
        obuf[s] = out[:heads, :head_dim]
        obuf[s + 1] = out[heads:, head_dim:]
        m_all = jnp.where(lane == b0, top[:heads], jnp.where(lane == b1, top[heads:], m_all))
        l_all = jnp.where(lane == b0, total[:heads], jnp.where(lane == b1, total[heads:], l_all))
        return m_all, l_all

    def step(i, carry):
        for part in parts:
            @pl.when((i >= LAG) & (i + NBUF - LAG < steps))
            def _():
                for cp in copies_out(i - LAG, part):
                    cp.wait()

            @pl.when(i + NBUF - LAG < steps)
            def _():
                for cp in copies_in(i + NBUF - LAG, part):
                    cp.start()

        m_all, l_all = mbuf[...], lbuf[...]
        for part in parts:
            for cp in copies_in(i, part):
                cp.wait()
            for s in range(part * PART, (part + 1) * PART):
                store_token(i, s)
            for s in range(part * PART, (part + 1) * PART, 2):
                m_all, l_all = attend_pair(i, s, m_all, l_all)
            for cp in copies_out(i, part):
                cp.start()
        mbuf[...] = m_all
        lbuf[...] = l_all
        out_rows = pl.ds(pl.multiple_of(i * CHUNK, CHUNK), CHUNK)
        by_head = jnp.swapaxes(obuf[...], 0, 1)
        own_ref[:half, out_rows] = jnp.where(core == 0, by_head[:half], by_head[half:])
        oth_ref[:half, out_rows] = jnp.where(core == 0, by_head[half:], by_head[:half])

        return carry

    mbuf[...] = jnp.zeros_like(mbuf)
    lbuf[...] = jnp.zeros_like(lbuf)
    for cp in small:
        cp.wait()
    lax.fori_loop(0, steps, step, 0)
    for i in range(steps - NBUF, steps):
        for part in parts:
            for cp in copies_out(i, part):
                cp.wait()
    stats = []
    for lo in (0, half):
        rows_ml = [mbuf[lo:lo + half], lbuf[lo:lo + half], jnp.zeros((batch - 2 * half, batch), jnp.float32)]
        stats.append(jnp.concatenate(rows_ml, axis=0).T[first:first + count])
    own_ref[half] = jnp.where(core == 0, stats[0], stats[1])
    oth_ref[half] = jnp.where(core == 0, stats[1], stats[0])


def write_and_attend(first, count, lengths, q_all, kv_all, k_cache, v_cache, written=()):
    batch, rows, head_dim = k_cache.shape
    heads = q_all.shape[0] * q_all.shape[2]
    part = jax.ShapeDtypeStruct((heads // 2 + 1, count, head_dim), jnp.float32)
    cache = jax.ShapeDtypeStruct(k_cache.shape, k_cache.dtype)
    return pl.pallas_call(
        functools.partial(attend_kernel, first, count),
        out_shape=(cache, cache, part, part),
        in_specs=[SMEM] + [HBM] * 4 + [ANY] * len(written),
        out_specs=(ANY, ANY, VMEM, VMEM),
        input_output_aliases={5: 0, 6: 1} if written else {},
        scratch_shapes=[
            pltpu.VMEM((2, count) + q_all.shape[2:], jnp.float32),
            pltpu.VMEM((2, count) + kv_all.shape[2:], jnp.float32),
            pltpu.VMEM((NBUF, CHUNK, rows, head_dim), jnp.bfloat16),
            pltpu.VMEM((NBUF, CHUNK, rows, head_dim), jnp.bfloat16),
            pltpu.VMEM((CHUNK, heads, head_dim), jnp.float32),
            pltpu.VMEM((heads, batch), jnp.float32),
            pltpu.VMEM((heads, batch), jnp.float32),
            pltpu.SemaphoreType.DMA((2, NBUF, CHUNK // PART)),
            pltpu.SemaphoreType.DMA((2, NBUF, CHUNK // PART)),
            pltpu.SemaphoreType.DMA((2,)),
        ],
        compiler_params=pltpu.CompilerParams(vmem_limit_bytes=34 * 1024 * 1024),
        cost_estimate=pl.CostEstimate(flops=100 * count * heads * rows * head_dim, bytes_accessed=8 * count * rows * head_dim, transcendentals=0),
        name='attend',
    )(lengths, q_all, kv_all, k_cache, v_cache, *written)


FIRST = 64
PIECES = (64, 48, 16)
UNITS = ((0, 32, 'Q'), (0, 32, 'Q'), (1, 24, 'P'), (1, 24, 'P'), (2, 16, 'D'))
ORDER = ('m0', 's0', 's1', 'h1', 'm1', 'h2', 'f0', 'f1', 's2', 'm2', 's3', 'f2', 's4',
         'f3', 'f4', 'l0', 'l1', 'l4', 'l2', 'e0', 'e1', 'e4', 'e2', 'l3', 'e3')
MESH = pl.DeviceIdType.MESH


def weigh(tiles):
    half = 16
    tops = [t[:, :half] for t in tiles]
    top = functools.reduce(jnp.maximum, tops)
    scales = [jnp.exp2(m - top) for m in tops]
    total = sum(t[:, half:2 * half] * s for t, s in zip(tiles, scales))
    return top, total, scales


def combine_kernel(own_a, core_a, x_a, diag_a, own_b, oth_b, w_hbm, hid_hbm, y_ref, w, hid, r1, c1, r2, att, lhs, part, r3, yall,
                   w_sem, send, recv):
    heads, batch, head_dim = att.shape
    half = heads // 2
    cols = part.shape[2]
    first = own_a.shape[1]
    pieces = [(sum(PIECES[:j]), n) for j, n in enumerate(PIECES)]
    count = len(pieces)
    units = [(sum(n for _, n, _ in UNITS[:u]), n) for u, (_, n, _) in enumerate(UNITS)]
    units_of = [[u for u, unit in enumerate(UNITS) if unit[0] == j] for j in range(count)]
    direct = [UNITS[us[0]][2] == 'D' for us in units_of]
    sp, y = lax.axis_index('sp'), lax.axis_index('tp')
    c, x = lax.rem(sp, 2), sp // 2
    to_c, to_x, to_y = {'sp': sp + 1 - 2 * c}, {'sp': sp + 2 - 4 * x}, {'tp': 1 - y}
    block = lambda xx, cc, yy: 4 * xx + 2 * cc + yy
    mine = block(x, c, y)

    barrier = pltpu.get_barrier_semaphore()
    for dev in (to_c, to_x, to_y):
        pl.semaphore_signal(barrier, inc=1, device_id=dev, device_id_type=MESH)

    def w_copy(h):
        return pltpu.make_async_copy(w_hbm.at[:, pl.ds(pl.multiple_of((2 * sp + h) * cols, cols), cols)], w.at[h], w_sem.at[h])

    def hid_copy(h):
        return pltpu.make_async_copy(hid_hbm.at[:, pl.ds(pl.multiple_of((2 * sp + h) * cols, cols), cols)], hid.at[h], w_sem.at[2 + h])

    w_copy(1 - y).start()
    pl.semaphore_wait(barrier, 3)

    def copy(kind, j, src, dst, dev):
        return pltpu.make_async_remote_copy(src_ref=src, dst_ref=dst, send_sem=send.at[kind, j], recv_sem=recv.at[kind, j], device_id=dev, device_id_type=MESH)

    def at(j):
        return pl.ds(*pieces[j])

    def local(j):
        return pl.ds(pieces[j][0] - first, pieces[j][1])

    pending = []

    def push(cp):
        cp.start()
        pending.append(cp)

    b_range = range(1, count)
    stat_c = copy(0, 0, oth_b.at[half], r1.at[half], to_c)
    push(stat_c)
    o_copies = {j: copy(1, j, oth_b.at[pl.ds(0, half), local(j)], r1.at[pl.ds(0, half), local(j)], to_c) for j in b_range}
    for j in b_range:
        push(o_copies[j])

    own_att = att.at[pl.ds(c * half, half)]
    att_copies = [copy(4, j, own_att.at[:, at(j)], own_att.at[:, at(j)], to_c) for j in range(count)]
    part_copies = [copy(5, u, part.at[1 - y, pl.ds(*unit)], r3.at[1 - y, pl.ds(*unit)], to_y) for u, unit in enumerate(units)]

    parts_a = (own_a, core_a, x_a, diag_a)
    _, total, scales = weigh([p[half] for p in parts_a])
    scales = [s / total for s in scales]
    for h in range(half):
        att[c * half + h, at(0)] = sum(p[h] * s[:, h:h + 1] for p, s in zip(parts_a, scales))
    push(att_copies[0])

    stat_c.wait_recv()
    top, total, scales = weigh([own_b[half], r1[half]])
    c1[half] = jnp.concatenate([top, total, jnp.zeros((own_b.shape[1], head_dim - 2 * half), jnp.float32)], axis=1)
    stat_x = copy(2, 0, c1.at[half], r2.at[half], to_x)
    push(stat_x)
    x_copies = {j: copy(3, j, c1.at[pl.ds(0, half), local(j)], r2.at[pl.ds(0, half), local(j)], to_x) for j in b_range}
    for j in b_range:
        o_copies[j].wait_recv()
        lo, n = pieces[j][0] - first, pieces[j][1]
        for h in range(half):
            c1[h, local(j)] = own_b[h, local(j)] * scales[0][lo:lo + n, h:h + 1] + r1[h, local(j)] * scales[1][lo:lo + n, h:h + 1]
        push(x_copies[j])
    w_copy(y).start()
    for h in range(2):
        hid_copy(h).start()

    def spread(kind, u, blk, dev):
        rows = pl.ds(*units[u])
        return copy(kind, u, yall.at[blk, rows], yall.at[blk, rows], dev)

    b_x, b_y, b_xy = block(1 - x, c, y), block(x, c, 1 - y), block(1 - x, c, 1 - y)
    final = {}

    def finish_heads(j):
        if j == 0:
            return
        if j == 1:
            stat_x.wait_recv()
            _, tot, sc = weigh([c1[half], r2[half]])
            final['scales'] = [s / tot for s in sc]
        x_copies[j].wait_recv()
        lo, n = pieces[j][0] - first, pieces[j][1]
        for h in range(half):
            att[c * half + h, at(j)] = sum(p[h, local(j)] * s[lo:lo + n, h:h + 1] for p, s in zip((c1, r2), final['scales']))
        push(att_copies[j])

    def multiply(j):
        att_copies[j].wait_recv()
        n = pieces[j][1]
        for h in range(heads):
            lhs[:n, h * head_dim:(h + 1) * head_dim] = att[h, at(j)].astype(jnp.bfloat16)

        def tiles(side):
            def tile(i, carry):
                sl = pl.ds(pl.multiple_of(i * 256, 256), 256)
                part[side, at(j), sl] = jnp.dot(lhs[:n], w[side, :, sl], preferred_element_type=jnp.float32)
                return carry
            lax.fori_loop(0, cols // 256, tile, 0)

        if j == 0:
            w_copy(1 - y).wait()
        tiles(1 - y)
        for u in units_of[j]:
            push(part_copies[u])
        if j == 0:
            w_copy(y).wait()
        tiles(y)
        if direct[j]:
            for u in units_of[j]:
                push(both_copy(u))

    def both_copy(u):
        return copy(13, u, part.at[y, pl.ds(*units[u])], r3.at[y, pl.ds(*units[u])], to_y)

    def finish_sum(u):
        if u == 0:
            for h in range(2):
                hid_copy(h).wait()
        rows = pl.ds(*units[u])
        part_copies[u].wait_recv()
        if UNITS[u][2] == 'D':
            both_copy(u).wait_recv()
            for side in range(2):
                yall[block(x, c, side), rows] = hid[side, rows].astype(jnp.float32) + (part[side, rows] + r3[side, rows])
            push(spread(7, u, mine, to_x))
            push(spread(10, u, b_y, to_x))
            push(spread(6, u, mine, to_c))
            push(spread(11, u, b_y, to_c))
            return
        yall[mine, rows] = hid[y, rows].astype(jnp.float32) + (part[y, rows] + r3[y, rows])
        push(spread(8, u, mine, to_y))
        push(spread(7, u, mine, to_x))
        push(spread(6, u, mine, to_c))

    def forward(u):
        mode = UNITS[u][2]

        def from_x():
            spread(7, u, b_x, to_x).wait_recv()
            if mode == 'P':
                push(spread(10, u, b_x, to_y))
            push(spread(9, u, b_x, to_c))

        def from_y():
            spread(8, u, b_y, to_y).wait_recv()
            if mode == 'Q':
                push(spread(10, u, b_y, to_x))
            push(spread(11, u, b_y, to_c))

        for take in {'P': (from_x, from_y), 'Q': (from_y, from_x), 'D': (from_x,)}[mode]:
            take()

    def forward_last(u):
        spread(10, u, b_xy, to_y).wait_recv()
        push(spread(12, u, b_xy, to_c))

    def emit(u):
        spread(6, u, block(x, 1 - c, y), to_c).wait_recv()
        spread(9, u, block(1 - x, 1 - c, y), to_c).wait_recv()
        spread(11, u, block(x, 1 - c, 1 - y), to_c).wait_recv()
        spread(12, u, block(1 - x, 1 - c, 1 - y), to_c).wait_recv()
        for g in range(8):
            y_ref[pl.ds(*units[u]), g * cols:(g + 1) * cols] = yall[g, pl.ds(*units[u])].astype(y_ref.dtype)

    stages = {'h': finish_heads, 's': finish_sum, 'm': multiply, 'f': forward, 'l': forward_last, 'e': emit}
    for name in ORDER:
        stages[name[0]](int(name[1:]))
    for cp in pending:
        cp.wait_send()


def combine_and_project(parts_a, parts_b, w_o, hidden):
    ext, nb_a, head_dim = parts_a[0].shape
    nb_b = parts_b[0].shape[1]
    batch = nb_a + nb_b
    half = ext - 1
    heads = 2 * half
    cols = w_o.shape[1] // 8
    f32 = jnp.float32
    kinds, count = 14, max(len(PIECES), len(UNITS))
    return pl.pallas_call(
        combine_kernel,
        out_shape=jax.ShapeDtypeStruct(hidden.shape, hidden.dtype),
        in_specs=[VMEM] * 6 + [ANY, ANY],
        out_specs=VMEM,
        scratch_shapes=[
            pltpu.VMEM((2, w_o.shape[0], cols), w_o.dtype),
            pltpu.VMEM((2, batch, cols), hidden.dtype),
            pltpu.VMEM((ext, nb_b, head_dim), f32),
            pltpu.VMEM((ext, nb_b, head_dim), f32),
            pltpu.VMEM((ext, nb_b, head_dim), f32),
            pltpu.VMEM((heads, batch, head_dim), f32),
            pltpu.VMEM((max(PIECES), heads * head_dim), jnp.bfloat16),
            pltpu.VMEM((2, batch, cols), f32),
            pltpu.VMEM((2, batch, cols), f32),
            pltpu.VMEM((8, batch, cols), f32),
            pltpu.SemaphoreType.DMA((4,)),
            pltpu.SemaphoreType.DMA((kinds, count)),
            pltpu.SemaphoreType.DMA((kinds, count)),
        ],
        compiler_params=pltpu.CompilerParams(collective_id=1, has_side_effects=True, vmem_limit_bytes=38 * 1024 * 1024),
        name='combine',
    )(*parts_a, *parts_b, w_o, hidden)


K_PIECES = 8
N_TILE = 1024
AHEAD = 8


def project_kernel(hid_hbm, gain_hbm, len_hbm, freq_hbm, wq_hbm, wk_hbm, wv_hbm, q_ref, kv_ref, hid_ref, gain_ref, len_ref, freq_ref, cos_ref, sin_ref, gain32, normed, acc, kv_acc, wbuf, kv_buf, hid_sem, w_sem, send, recv):
    batch, depth = hid_ref.shape
    head_dim = cos_ref.shape[1]
    q_cols = wq_hbm.shape[1] // 2
    kv_cols = wk_hbm.shape[1]
    k_rows = depth // K_PIECES
    q_tiles = q_cols // N_TILE
    sp = lax.axis_index('sp')
    c = lax.rem(sp, 2)
    to_c = {'sp': sp + 1 - 2 * c}

    barrier = pltpu.get_barrier_semaphore()
    pl.semaphore_signal(barrier, inc=1, device_id=to_c, device_id_type=MESH)

    def fetch(n, k):
        rows = pl.ds(k * k_rows, k_rows)
        if n == q_tiles:
            return tuple(pltpu.make_async_copy(src.at[rows], kv_buf.at[k], w_sem.at[n, k]) for src in (wk_hbm, wv_hbm))
        col = pl.ds(pl.multiple_of(c * q_cols + n * N_TILE, N_TILE), N_TILE)
        return (pltpu.make_async_copy(wq_hbm.at[rows, col], wbuf.at[n, k], w_sem.at[n, k]),)

    def start(n, k):
        cps = fetch(n, k)
        if n < q_tiles:
            cps[0].start()
            return
        for core in range(2):
            @pl.when(c == core)
            def _(core=core):
                cps[core].start()

    small = [pltpu.make_async_copy(src, dst, hid_sem.at[i]) for i, (src, dst) in enumerate(
        ((hid_hbm, hid_ref), (gain_hbm, gain_ref), (len_hbm, len_ref), (freq_hbm, freq_ref)))]
    for cp in small:
        cp.start()
    order = [piece for k in range(K_PIECES) for piece in ((0, k), (q_tiles, k))]
    order += [(n, k) for n in range(1, q_tiles) for k in range(K_PIECES)]
    for piece in order[:AHEAD]:
        start(*piece)

    def angle_tables():
        angles = jnp.broadcast_to(len_ref[...].astype(jnp.float32), (batch, batch)).T[:, :head_dim] * jnp.concatenate([freq_ref[...]] * 2, axis=1)
        sin_ang = jnp.sin(angles)
        cos_ref[...] = jnp.cos(angles)
        sin_ref[...] = jnp.where(lax.broadcasted_iota(jnp.int32, angles.shape, 1) < head_dim // 2, -sin_ang, sin_ang)

    for cp in small:
        cp.wait()
    gain32[...] = gain_ref[...].astype(jnp.float32)
    step = 1024
    total = jnp.zeros((batch, 1), jnp.float32)
    for j in range(depth // step):
        part = hid_ref[:, j * step:(j + 1) * step].astype(jnp.float32)
        total = total + jnp.sum(part * part, axis=-1, keepdims=True)
    inv_rms = lax.rsqrt(total / depth + NORM_EPS)
    lanes = gain_ref.shape[1]

    def normalize(k):
        for j in range(k * k_rows // lanes, (k + 1) * k_rows // lanes):
            sl = slice(j * lanes, (j + 1) * lanes)
            normed[:, sl] = (hid_ref[:, sl].astype(jnp.float32) * inv_rms * gain32[j:j + 1, :]).astype(normed.dtype)

    def round_bf16(v):
        return v.astype(jnp.bfloat16).astype(jnp.float32)

    def rope(v):
        return round_bf16(v * cos_ref[...] + pltpu.roll(v, head_dim // 2, 1) * sin_ref[...])

    sends = []

    def push(slot, ref, index):
        cp = pltpu.make_async_remote_copy(src_ref=ref.at[index], dst_ref=ref.at[index], send_sem=send.at[slot], recv_sem=recv.at[slot], device_id=to_c, device_id_type=MESH)
        if not sends:
            pl.semaphore_wait(barrier, 1)
        cp.start()
        sends.append(cp)

    per = N_TILE // head_dim

    def epilogue_kv():
        for h in range(kv_cols // head_dim):
            v = round_bf16(kv_acc[:, h * head_dim:(h + 1) * head_dim])
            kv_ref[c, :, h, :] = jnp.where(c == 0, rope(v), v)
        push(q_tiles, kv_ref, c)

    def epilogue(n):
        for h in range(per):
            q_ref[c, :, n * per + h, :] = rope(round_bf16(acc[n % 2, :, h * head_dim:(h + 1) * head_dim]))
        push(n, q_ref, (c, slice(None), pl.ds(n * per, per)))

    for i, (n, k) in enumerate(order):
        fetch(n, k)[0].wait()
        if i + AHEAD < len(order):
            start(*order[i + AHEAD])
        if n == 0:
            normalize(k)
        lhs = normed[:, k * k_rows:(k + 1) * k_rows]
        if n == q_tiles:
            prod = jnp.dot(lhs, kv_buf[k], preferred_element_type=jnp.float32)
            kv_acc[...] = prod + kv_acc[...] if k else prod
        else:
            prod = jnp.dot(lhs, wbuf[n, k], preferred_element_type=jnp.float32)
            acc[n % 2] = prod + acc[n % 2] if k else prod
        if (n, k) == (0, 3):
            angle_tables()
        if (n, k) == (1, 1):
            epilogue_kv()
        if 0 < n < q_tiles and k == 2:
            epilogue(n - 1)
    epilogue(q_tiles - 1)
    for cp in sends:
        cp.wait()


def project(hidden, lengths, norm_gain, w_q, w_k, w_v, inv_freq):
    batch, depth = hidden.shape
    head_dim = 2 * inv_freq.shape[0]
    q_heads = w_q.shape[1] // 2 // head_dim
    kv_heads = w_k.shape[1] // head_dim
    q_tiles = w_q.shape[1] // 2 // N_TILE
    return pl.pallas_call(
        project_kernel,
        out_shape=(jax.ShapeDtypeStruct((2, batch, q_heads, head_dim), jnp.float32), jax.ShapeDtypeStruct((2, batch, kv_heads, head_dim), jnp.float32)),
        in_specs=[HBM] * 7,
        out_specs=(VMEM, VMEM),
        scratch_shapes=[
            pltpu.VMEM((batch, depth), hidden.dtype),
            pltpu.VMEM((depth // 128, 128), norm_gain.dtype),
            pltpu.VMEM((1, batch), jnp.int32),
            pltpu.VMEM((1, head_dim // 2), jnp.float32),
            pltpu.VMEM((batch, head_dim), jnp.float32),
            pltpu.VMEM((batch, head_dim), jnp.float32),
            pltpu.VMEM((depth // 128, 128), jnp.float32),
            pltpu.VMEM((batch, depth), jnp.bfloat16),
            pltpu.VMEM((2, batch, N_TILE), jnp.float32),
            pltpu.VMEM((batch, w_k.shape[1]), jnp.float32),
            pltpu.VMEM((q_tiles, K_PIECES, depth // K_PIECES, N_TILE), w_q.dtype),
            pltpu.VMEM((K_PIECES, depth // K_PIECES, w_k.shape[1]), w_k.dtype),
            pltpu.SemaphoreType.DMA((4,)),
            pltpu.SemaphoreType.DMA((q_tiles + 1, K_PIECES)),
            pltpu.SemaphoreType.DMA((q_tiles + 1,)),
            pltpu.SemaphoreType.DMA((q_tiles + 1,)),
        ],
        compiler_params=pltpu.CompilerParams(collective_id=0, has_side_effects=True, vmem_limit_bytes=50 * 1024 * 1024),
        name='project',
    )(hidden, norm_gain.reshape(depth // 128, 128), lengths.reshape(1, batch), inv_freq.reshape(1, head_dim // 2), w_q, w_k, w_v)


def device_step(hidden, lengths, k_cache, v_cache, norm_gain, w_q, w_k, w_v, w_o, inv_freq):
    batch, slots, kv_local, head_dim = k_cache.shape
    q_all, kv_all = project(hidden, lengths, norm_gain, w_q, w_k, w_v, inv_freq)
    flat = (batch, slots * kv_local, head_dim)
    shared = (lengths, q_all, kv_all, k_cache.reshape(flat), v_cache.reshape(flat))
    k_upd, v_upd, own_a, oth_a = write_and_attend(0, FIRST, *shared)
    swap = lambda array, flip: lax.ppermute(array, 'sp', [(s, s ^ flip) for s in range(4)])
    parts_a = (own_a, swap(oth_a, 1), swap(own_a, 2), swap(oth_a, 3))
    k_upd, v_upd, own_b, oth_b = write_and_attend(FIRST, batch - FIRST, *shared, written=(k_upd, v_upd))
    y_out = combine_and_project(parts_a, (own_b, oth_b), w_o, hidden)
    return y_out, k_upd.reshape(k_cache.shape), v_upd.reshape(v_cache.shape)


def solution(mesh):
    cache_spec = P('dp', 'sp', 'tp', None)
    in_specs = (P('dp', None), P('dp'), cache_spec, cache_spec, P(None), P(None, 'tp'), P(None, 'tp'), P(None, 'tp'), P('tp', None), P(None))
    out_specs = (P('dp', None), cache_spec, cache_spec)
    return jax.shard_map(device_step, mesh=mesh, in_specs=in_specs, out_specs=out_specs, check_vma=False)
```
